256 devices in a mesh: seq: 64 (over y, x_lo, z), dp: 4 (over x_hi, core).
Axes of the slice: x: 4 (x_hi: 2, x_lo: 2; x = x_hi * 2 + x_lo), y: 4, z: 8, core: 2. Of those that a mesh axis runs over, the one named last changes fastest.
Arguments:
- queries: bfloat16 [4, 16384, 2048], P('dp', 'seq'), may hold values from -12 to 12
- keys: bfloat16 [4, 16384, 1024], P('dp', 'seq'), may hold values from -6 to 6
- values: bfloat16 [4, 16384, 1024], P('dp', 'seq'), may hold values from -6 to 6
- out_grad: bfloat16 [4, 16384, 1792], P('dp', 'seq'), may hold values from -6 to 6
- out_weight: bfloat16 [2048, 1792], P('seq'), may hold values from -0.125 to 0.125
- seq_len: int32 [4], P('dp'), may hold values from 4096 to 16384, as said below
Outputs:
- query_grad: bfloat16 [4, 16384, 2048], P('dp', 'seq')
- key_grad: bfloat16 [4, 16384, 1024], P('dp', 'seq')
- value_grad: bfloat16 [4, 16384, 1024], P('dp', 'seq')
- weight_grad: float32 [2048, 1792], P('seq')
- grad_rms: float32 [], replicated
The draws below stay inside these ranges and needn't reach their ends.
Inputs may be any that keep to these rules, and one draw needn't show every extreme that they name: `seq_len`: at least one sequence has the full length 16384.
All inputs are finite; a program needn't handle non-finite values.
Results may differ from the reference program's by a relative error of at most 0.014.
Values may be sent and summed in bfloat16 or wider, within the bound.
A program may use at most 128 MiB of HBM per device.

```python
import jax
import jax.numpy as jnp
from jax import lax

HEADS = 8
KV_HEADS = 4
HEAD_DIM = 256
D_OUT = 1792
WINDOW = 512
TOK_DEV = 256
SEQ = 16384
N_SEQ = 64
N_DP = 4


def draw_seq_len(key, part):
    total = TOK_DEV * N_SEQ
    lengths = jax.random.randint(jax.random.fold_in(key, 11), (N_DP,), total // 4, total + 1, dtype=jnp.int32)
    chosen = jax.random.randint(jax.random.fold_in(key, 12), (), 0, N_DP, dtype=jnp.int32)
    places = jnp.arange(N_DP, dtype=jnp.int32)
    return jnp.where(places == chosen, jnp.int32(total), lengths).astype(jnp.int32)


def level_of(rng, extent, cuts, least, top_value):
    loudness, own = 1.0, jax.random.fold_in(rng, 6)
    for axis_at, shards_of in cuts:
        draws = jnp.exp(jax.random.uniform(jax.random.fold_in(own, axis_at), (shards_of,), jnp.float32, least / len(cuts), top_value / len(cuts)))
        loudness = loudness * jnp.repeat(draws, extent[axis_at] // shards_of).reshape([-1 if axis == axis_at else 1 for axis in range(len(extent))])
    return loudness


def scatter_about(stream_key, dims, width, most, split=(), kind=jnp.bfloat16):
    values = jax.random.normal(stream_key, dims, jnp.float32) * width
    if len(split) > 0:
        values = level_of(stream_key, dims, split, -0.22, 0.18) * values
    return jnp.clip(values, min=-most, max=most).astype(kind)


def setup_inputs(seed: int = 0) -> dict:
    arg_keys = jax.random.split(jax.random.key(seed), 7)
    queries = scatter_about(arg_keys[0], (N_DP, SEQ, HEADS * HEAD_DIM), 2.0, 12.0, ((0, 4), (1, 64)))
    keys = scatter_about(arg_keys[1], (N_DP, SEQ, KV_HEADS * HEAD_DIM), 1.0, 6.0, ((0, 4), (1, 64)))
    values = scatter_about(arg_keys[2], (N_DP, SEQ, KV_HEADS * HEAD_DIM), 1.0, 6.0, ((0, 4), (1, 64)))
    out_grad = scatter_about(arg_keys[3], (N_DP, SEQ, D_OUT), 1.0, 6.0, ((0, 4), (1, 64)))
    out_weight = scatter_about(arg_keys[4], (HEADS * HEAD_DIM, D_OUT), (HEADS * HEAD_DIM) ** -0.5, 0.125, ((0, 64),))
    seq_len = draw_seq_len(jax.random.fold_in(arg_keys[6], 71), 0)
    return {"queries": queries, "keys": keys, "values": values, "out_grad": out_grad, "out_weight": out_weight, "seq_len": seq_len}


SCALE = 0.0625
CAP = 50.0

def band_block(q_rows, k_rows, v_rows, g_rows, q_pos, k_pos):
    count = q_rows.shape[0]
    span = k_rows.shape[0]
    group = HEADS // KV_HEADS
    qh = q_rows.astype(jnp.float32).reshape(count, KV_HEADS, group, HEAD_DIM)
    kh = k_rows.astype(jnp.float32).reshape(span, KV_HEADS, HEAD_DIM)
    vh = v_rows.astype(jnp.float32).reshape(span, KV_HEADS, HEAD_DIM)
    gh = g_rows.astype(jnp.float32).reshape(count, KV_HEADS, group, HEAD_DIM)
    raw = jnp.einsum('tkgd,jkd->kgtj', qh, kh) * SCALE
    capped = CAP * jnp.tanh(raw / CAP)
    allowed = (k_pos[None, :] >= 0) & (k_pos[None, :] <= q_pos[:, None]) & (k_pos[None, :] > q_pos[:, None] - WINDOW)
    expo = jnp.where(allowed, jnp.exp(capped), jnp.zeros((), jnp.float32))
    probs = expo / lax.optimization_barrier(jnp.sum(expo, axis=-1, keepdims=True))
    probs_b = probs.astype(jnp.bfloat16)
    attn = jnp.einsum('kgtj,jkd->tkgd', probs_b.astype(jnp.float32), vh).astype(jnp.bfloat16)
    delta = jnp.einsum('tkgd,tkgd->kgt', gh, attn.astype(jnp.float32))[..., None]
    dprob = jnp.einsum('tkgd,jkd->kgtj', gh, vh)
    dscore = (probs * (dprob - delta) * (1.0 - (capped / CAP) ** 2) * SCALE).astype(jnp.bfloat16)
    dscore32 = dscore.astype(jnp.float32)
    dq = jnp.einsum('kgtj,jkd->tkgd', dscore32, kh).reshape(count, -1)
    dk = jnp.einsum('kgtj,tkgd->jkd', dscore32, qh).reshape(span, -1)
    dv = jnp.einsum('kgtj,tkgd->jkd', probs_b.astype(jnp.float32), gh).reshape(span, -1)
    return (dq, dk, dv, attn.reshape(count, -1))

def reference(queries, keys, values, out_grad, out_weight, seq_len):
    seq = TOK_DEV * N_SEQ
    reach = (WINDOW + TOK_DEV - 2) // TOK_DEV
    lead = reach * TOK_DEV
    span = lead + TOK_DEV
    kv_width = KV_HEADS * HEAD_DIM
    q_list = []
    k_list = []
    v_list = []
    weight_raw = jnp.zeros((HEADS * HEAD_DIM, D_OUT), jnp.float32)
    count = jnp.zeros((), jnp.int32)
    for rep in range(N_DP):
        length = seq_len[rep]
        positions = jnp.arange(seq, dtype=jnp.int32)
        valid = positions < length
        masked = jnp.where(valid[:, None], out_grad[rep], jnp.zeros((), jnp.bfloat16))
        grad_attn = jnp.dot(masked, out_weight.T, preferred_element_type=jnp.float32).astype(jnp.bfloat16)
        blank = jnp.zeros((lead, kv_width), jnp.bfloat16)
        key_pad = jnp.concatenate([blank, keys[rep]], 0)
        val_pad = jnp.concatenate([blank, values[rep]], 0)
        rep_queries = queries[rep]

        def step(carry, block):
            dk_pad, dv_pad = carry
            first = (block * TOK_DEV).astype(jnp.int32)
            q_rows = lax.dynamic_slice_in_dim(rep_queries, first, TOK_DEV, 0)
            g_rows = lax.dynamic_slice_in_dim(grad_attn, first, TOK_DEV, 0)
            k_rows = lax.dynamic_slice_in_dim(key_pad, first, span, 0)
            v_rows = lax.dynamic_slice_in_dim(val_pad, first, span, 0)
            q_pos = first + jnp.arange(TOK_DEV, dtype=jnp.int32)
            k_pos = first - lead + jnp.arange(span, dtype=jnp.int32)
            dq, dk, dv, attn = band_block(q_rows, k_rows, v_rows, g_rows, q_pos, k_pos)
            dk_pad = lax.dynamic_update_slice_in_dim(dk_pad, lax.dynamic_slice_in_dim(dk_pad, first, span, 0) + dk, first, 0)
            dv_pad = lax.dynamic_update_slice_in_dim(dv_pad, lax.dynamic_slice_in_dim(dv_pad, first, span, 0) + dv, first, 0)
            return ((dk_pad, dv_pad), (dq, attn))
        init = (jnp.zeros((seq + lead, kv_width), jnp.float32), jnp.zeros((seq + lead, kv_width), jnp.float32))
        (dk_pad, dv_pad), (dq_blocks, attn_blocks) = lax.scan(step, init, jnp.arange(N_SEQ, dtype=jnp.int32))
        q_list.append(dq_blocks.reshape(seq, -1))
        k_list.append(dk_pad[lead:])
        v_list.append(dv_pad[lead:])
        attn_full = attn_blocks.reshape(seq, -1)
        weight_raw = weight_raw + jnp.dot(attn_full.T, masked, preferred_element_type=jnp.float32)
        count = count + jnp.sum(valid.astype(jnp.int32))
    total = count.astype(jnp.float32)
    act_scale = N_DP * seq / total
    weight_scale = lax.rsqrt(total)
    dq_all = jnp.stack(q_list) * act_scale
    dk_all = jnp.stack(k_list) * act_scale
    dv_all = jnp.stack(v_list) * act_scale
    weight_grad = weight_raw * weight_scale
    squares = jnp.sum(dq_all * dq_all) + jnp.sum(dk_all * dk_all) + jnp.sum(dv_all * dv_all) + jnp.sum(weight_grad * weight_grad)
    entries = N_DP * seq * (HEADS + 2 * KV_HEADS) * HEAD_DIM + HEADS * HEAD_DIM * D_OUT
    grad_rms = jnp.sqrt(squares / entries)
    return (dq_all.astype(jnp.bfloat16), dk_all.astype(jnp.bfloat16), dv_all.astype(jnp.bfloat16), weight_grad, grad_rms)
```

```python
import functools

import jax
import jax.numpy as jnp
from jax import lax
from jax.experimental import pallas as pl
from jax.experimental.pallas import tpu as pltpu
from jax.sharding import Mesh
from jax.sharding import PartitionSpec as P

HEADS = 8
KV_HEADS = 4
GROUP = HEADS // KV_HEADS
HD = 256
D_OUT = 1792
WINDOW = 512
TOK = 256
SEQ = ("sy", "sx", "sz")
DP = ("dx", "dc")
AXES = ("sy", "sx", "sz", "dx", "dc")
N_DEV_SEQ = 64
SLOTS = 4 * 16384

SCALE = 0.0625
CAP = 50.0
LOG2E = 1.4426950408889634
CHANNELS = 128

F32 = jnp.float32
BF16 = jnp.bfloat16
MESH = pl.DeviceIdType.MESH


def dot_nt(a, b):
    return lax.dot_general(a, b, (((1,), (1,)), ((), ())), preferred_element_type=F32)


def dot_nn(a, b):
    return lax.dot_general(a, b, (((1,), (0,)), ((), ())), preferred_element_type=F32)


def dot_tn(a, b):
    return lax.dot_general(a, b, (((0,), (0,)), ((), ())), preferred_element_type=F32)


def col(n):
    return pl.ds(n * HD, HD)


def body(
    len_ref, q_ref, k_ref, v_ref, og_ref, w_ref, lt_ref,
    dq_ref, dk_ref, dv_ref, dw_ref, sq_ref,
    wf, k1, k2, v1, v2, mk, at, pb, pw, tw, dwm, sdb, rdb, xsb, xrb, ysb, yrb, zsb, zrb,
    fsb, frb, hsb, hrb, c2s, c2r, cms, cmr, c1, c0, lts, ssem, rsem,
):
    y, xl, z, xh, c = (lax.axis_index(a) for a in AXES)
    oc = 1 - c
    pos = (y * 2 + xl) * 8 + z

    def at_seq(s):
        return (lax.div(s, 16), lax.rem(lax.div(s, 8), 2), lax.rem(s, 8), xh, c)

    def mod(a, n):
        return lax.rem(a, n)

    right = at_seq(mod(pos + 1, N_DEV_SEQ))
    left = at_seq(mod(pos + N_DEV_SEQ - 1, N_DEV_SEQ))
    yn = (mod(y + 1, 4), xl, z, xh, c)
    yp = (mod(y + 3, 4), xl, z, xh, c)
    xr = (y, 1 - xl, z, mod(xh + xl, 2), c)
    xp = (y, 1 - xl, z, mod(xh + 1 - xl, 2), c)
    x2 = (y, xl, z, 1 - xh, c)
    x2o = (y, xl, z, 1 - xh, oc)
    cp = (y, xl, z, xh, oc)

    def zpeer(k):
        return (y, xl, mod(z + k, 8), xh, c)

    ids = {}
    sent = []

    def channel(name):
        return ids.setdefault(name, len(ids))

    def send(name, src, dst, dev):
        n = channel(name)
        d = pltpu.make_async_remote_copy(
            src_ref=src, dst_ref=dst, send_sem=ssem.at[n], recv_sem=rsem.at[n],
            device_id=dev, device_id_type=MESH,
        )
        d.start()
        sent.append(d)

    def recv(name, dst):
        n = channel(name)
        pltpu.make_async_remote_copy(
            src_ref=dst, dst_ref=dst, send_sem=ssem.at[n], recv_sem=rsem.at[n],
            device_id=cp, device_id_type=MESH,
        ).wait_recv()

    barrier = pltpu.get_barrier_semaphore()
    peers = [zpeer(k) for k in range(1, 8)] + [right, left, yn, yp, xr, xp, x2, x2o, cp]
    for dev in peers:
        pl.semaphore_signal(barrier, inc=1, device_id=dev, device_id_type=MESH)
    pl.semaphore_wait(barrier, len(peers))

    def unit(j):
        return mod(y + j, 4) * 2 + xl

    def other(j):
        return mod(y + j, 4) * 2 + 1 - xl

    def part(u, p, h):
        return wf.at[pl.ds(8 * u + 4 * p, 4), h]

    def x_dev(p):
        return xr if p == 0 else xp

    def spread(j, p):
        ref = part(unit(j), p, c)
        send(f"x{j}{p}", ref, ref, x_dev(p))
        send(f"d{j}{p}", ref, ref, cp)

    def gather_z():
        for k in range(1, 8):
            send(f"z{k}", w_ref.at[c], wf.at[pos, c], zpeer(k))
        wf[pos, c] = w_ref[c]

    def gather_y():
        for k in range(1, 8):
            recv(f"z{k}", wf.at[pos - z + mod(z + 8 - k, 8), c])
        for p in range(2):
            ref = part(unit(0), p, c)
            send(f"ya{p}", ref, ref, yn)
            send(f"yb{p}", ref, ref, yp)
        for p in range(2):
            spread(0, p)

    def gather_y0():
        recv("ya0", part(unit(3), 0, c))
        ref = part(unit(3), 0, c)
        send("yf0", ref, ref, yn)
        spread(3, 0)
        recv("yb0", part(unit(1), 0, c))
        spread(1, 0)

    def gather_y1():
        recv("yb1", part(unit(1), 1, c))
        ref = part(unit(1), 1, c)
        send("yf1", ref, ref, yp)
        spread(1, 1)
        recv("ya1", part(unit(3), 1, c))
        spread(3, 1)

    def gather_y2():
        for p in range(2):
            recv(f"yf{p}", part(unit(2), p, c))
            spread(2, p)

    def gather_x(j):
        for p in range(2):
            ref = part(other(j), p, c)
            recv(f"x{j}{p}", ref)
            send(f"e{j}{p}", ref, ref, cp)

    def gather_done():
        for j in range(4):
            for p in range(2):
                recv(f"d{j}{p}", part(unit(j), p, oc))
                recv(f"e{j}{p}", part(other(j), p, oc))

    def halo_own(kh):
        send(f"ok{kh}", k_ref.at[:, col(kh)], k1.at[:, col(kh)], right)
        send(f"ov{kh}", v_ref.at[:, col(kh)], v1.at[:, col(kh)], right)

    def halo_relay(kh):
        recv(f"ok{kh}", k1.at[:, col(kh)])
        send(f"fk{kh}", k1.at[:, col(kh)], k2.at[:, col(kh)], right)
        recv(f"ov{kh}", v1.at[:, col(kh)])
        send(f"fv{kh}", v1.at[:, col(kh)], v2.at[:, col(kh)], right)

    def halo_last(kh):
        recv(f"fk{kh}", k2.at[:, col(kh)])
        recv(f"fv{kh}", v2.at[:, col(kh)])

    def lengths_send():
        send("l0", lt_ref, lts.at[0], cp)
        send("l1", lt_ref, lts.at[1], x2)
        send("l2", lt_ref, lts.at[2], x2o)

    def lengths():
        for n in range(3):
            recv(f"l{n}", lts.at[n])
        total = (lt_ref[...] + lts[0] + lts[1] + lts[2]).astype(F32)[0:1, 0:1]
        return SLOTS / total, lax.rsqrt(total)

    def masked():
        row = lax.broadcasted_iota(jnp.int32, (TOK, 1), 0)
        mk[...] = jnp.where(row < len_ref[0] - pos * TOK, og_ref[...], jnp.zeros((), BF16))

    def forward(h):
        kh = h // GROUP
        q = q_ref[:, col(h)]
        row = lax.broadcasted_iota(jnp.int32, (TOK, TOK), 0)
        cl = lax.broadcasted_iota(jnp.int32, (TOK, TOK), 1)
        far = jnp.where(pos >= 2, 0, 2 * TOK)
        near = jnp.where(pos >= 1, 0, 2 * TOK)
        allowed = (cl - row > far, cl >= near, cl <= row)
        es, ws = [], []
        total = jnp.zeros((TOK, 1), F32)
        for b, ref in enumerate((k2, k1, k_ref)):
            t = jnp.tanh(dot_nt(q, ref[:, col(kh)]) * (SCALE / CAP))
            e = jnp.where(allowed[b], jnp.exp2(t * (CAP * LOG2E)), 0.0)
            total = total + jnp.sum(e, axis=1, keepdims=True)
            es.append(e)
            ws.append(e * (SCALE - SCALE * (t * t)))
        inv = 1.0 / total
        out = jnp.zeros((TOK, HD), F32)
        for b, ref in enumerate((v2, v1, v_ref)):
            p = (es[b] * inv).astype(BF16)
            pb[h, b] = p
            pw[h, b] = (ws[b] * inv).astype(BF16)
            out = out + dot_nn(p, ref[:, col(kh)])
        at[:, col(h)] = out.astype(BF16)

    def weight_part(h):
        tw[...] = dot_tn(at[:, col(h)], mk[...]).reshape(8, 2, 16, D_OUT)
        sdb[h] = tw[:, oc].astype(BF16)
        dwm[h] = tw[:, c]
        send(f"rd{h}", sdb.at[h], rdb.at[h], cp)

    def forward_pair(kh):
        for g in range(GROUP):
            forward(kh * GROUP + g)
            weight_part(kh * GROUP + g)

    def reduce_x(kh):
        for g in range(GROUP):
            h = kh * GROUP + g
            recv(f"rd{h}", rdb.at[h])
        u, o = kh * 2 + xl, kh * 2 + 1 - xl
        xsb[kh] = (dwm[o] + rdb[o].astype(F32)).astype(BF16)
        dwm[u] = dwm[u] + rdb[u].astype(F32)
        for p in range(2):
            send(f"rx{kh}{p}", xsb.at[kh, pl.ds(4 * p, 4)], xrb.at[kh, pl.ds(4 * p, 4)], x_dev(p))

    def reduce_x_done(kh):
        for p in range(2):
            recv(f"rx{kh}{p}", xrb.at[kh, pl.ds(4 * p, 4)])
        u = kh * 2 + xl
        dwm[u] = dwm[u] + xrb[kh].astype(F32)

    def mine(j, p):
        return dwm[unit(j), pl.ds(4 * p, 4)]

    def y_send(n, value, dev):
        ysb[n] = value.astype(BF16)
        send(f"r{n}", ysb.at[n], yrb.at[n], dev)

    def reduce_y():
        y_send(0, mine(2, 0), yn)
        y_send(1, mine(2, 1), yp)
        y_send(2, mine(1, 1), yn)
        y_send(3, mine(3, 0), yp)

    def reduce_y2():
        recv("r0", yrb.at[0])
        y_send(4, mine(1, 0) + yrb[0].astype(F32), yn)
        recv("r1", yrb.at[1])
        y_send(5, mine(3, 1) + yrb[1].astype(F32), yp)

    def reduce_z():
        for n in range(2, 6):
            recv(f"r{n}", yrb.at[n])
        u = unit(0)
        lo = mine(0, 0) + yrb[3].astype(F32) + yrb[4].astype(F32)
        hi = mine(0, 1) + yrb[2].astype(F32) + yrb[5].astype(F32)
        dwm[u, pl.ds(0, 4)] = lo
        dwm[u, pl.ds(4, 4)] = hi
        zsb[pl.ds(0, 4)] = lo.astype(BF16)
        zsb[pl.ds(4, 4)] = hi.astype(BF16)
        for k in range(1, 8):
            send(f"rz{k}", zsb.at[mod(z + k, 8)], zrb.at[k], zpeer(k))

    def reduce_dp():
        total = dwm[unit(0), z]
        for k in range(1, 8):
            recv(f"rz{k}", zrb.at[k])
            total = total + zrb[k].astype(F32)
        fsb[...] = total.astype(BF16)
        send("f", fsb, frb, x2)

    def reduce_swap(weight_scale):
        recv("f", frb)
        total = (fsb[...].astype(F32) + frb[...].astype(F32)) * weight_scale
        hsb[...] = total
        send("h", hsb, hrb, cp)
        dw_ref[c] = total
        square = total * total * 0.5
        acc = sq_ref[...]
        for n in range(D_OUT // HD):
            acc = acc + square[0:8, n * HD : (n + 1) * HD] + square[8:16, n * HD : (n + 1) * HD]
        sq_ref[...] = acc

    def reduce_end():
        recv("h", hrb)
        dw_ref[oc] = hrb[...]

    def squares(x):
        sq_ref[...] += jnp.sum((x * x).reshape(TOK // 8, 8, HD), axis=0)

    def backward(kh, act_scale):
        sk = [None] * 3
        sv = [None] * 3
        for g in range(GROUP):
            h = kh * GROUP + g
            q = q_ref[:, col(h)]
            wh = wf[pl.ds(8 * h, 8)].reshape(HD, D_OUT)
            ga = dot_nt(mk[...], wh).astype(BF16)
            delta = jnp.sum(ga.astype(F32) * at[:, col(h)].astype(F32), axis=1, keepdims=True)
            dq = jnp.zeros((TOK, HD), F32)
            for b, (kr, vr) in enumerate(((k2, v2), (k1, v1), (k_ref, v_ref))):
                dp = dot_nt(ga, vr[:, col(kh)])
                ds = (pw[h, b].astype(F32) * (dp - delta)).astype(BF16)
                dq = dq + dot_nn(ds, kr[:, col(kh)])
                dk = dot_tn(ds, q)
                dv = dot_tn(pb[h, b], ga)
                sk[b] = dk if g == 0 else sk[b] + dk
                sv[b] = dv if g == 0 else sv[b] + dv
            dq = dq * act_scale
            squares(dq)
            dq_ref[:, col(h)] = dq.astype(BF16)
        c2s[kh, 0] = sk[0].astype(BF16)
        c2s[kh, 1] = sv[0].astype(BF16)
        send(f"b{kh}", c2s.at[kh], c2r.at[kh], left)
        c1[kh, 0] = sk[1]
        c1[kh, 1] = sv[1]
        c0[kh, 0] = sk[2]
        c0[kh, 1] = sv[2]

    def combine(kh):
        recv(f"b{kh}", c2r.at[kh])
        cms[kh] = (c1[kh] + c2r[kh].astype(F32)).astype(BF16)
        send(f"m{kh}", cms.at[kh], cmr.at[kh], left)

    def finish(kh, act_scale):
        recv(f"m{kh}", cmr.at[kh])
        for n, ref in enumerate((dk_ref, dv_ref)):
            total = (c0[kh, n] + cmr[kh, n].astype(F32)) * act_scale
            squares(total)
            ref[:, col(kh)] = total.astype(BF16)

    sq_ref[...] = jnp.zeros_like(sq_ref)
    gather_z()
    lengths_send()
    halo_own(0)
    halo_own(1)
    masked()
    gather_y()
    act_scale, weight_scale = lengths()
    halo_relay(0)
    halo_own(2)
    gather_y0()
    gather_y1()
    halo_last(0)
    forward_pair(0)
    gather_y2()
    halo_relay(1)
    halo_own(3)
    for j in (0, 1, 3, 2):
        gather_x(j)
    reduce_x(0)
    gather_done()
    backward(0, act_scale)
    halo_last(1)
    forward_pair(1)
    halo_relay(2)
    backward(1, act_scale)
    combine(0)
    halo_last(2)
    reduce_x_done(0)
    reduce_x(1)
    forward_pair(2)
    halo_relay(3)
    backward(2, act_scale)
    combine(1)
    finish(0, act_scale)
    reduce_x_done(1)
    reduce_x(2)
    halo_last(3)
    forward_pair(3)
    reduce_x_done(2)
    reduce_x(3)
    backward(3, act_scale)
    combine(2)
    finish(1, act_scale)
    reduce_x_done(3)
    reduce_y()
    reduce_y2()
    combine(3)
    finish(2, act_scale)
    reduce_z()
    reduce_dp()
    reduce_swap(weight_scale)
    finish(3, act_scale)
    reduce_end()
    for d in sent:
        d.wait_send()


def shards(queries, keys, values, out_grad, out_weight, seq_len):
    vm = pl.BlockSpec(memory_space=pltpu.VMEM)
    scratch = [
        ((64, 2, 16, D_OUT), BF16),
        ((TOK, 1024), BF16),
        ((TOK, 1024), BF16),
        ((TOK, 1024), BF16),
        ((TOK, 1024), BF16),
        ((TOK, D_OUT), BF16),
        ((TOK, 2048), BF16),
        ((HEADS, 3, TOK, TOK), BF16),
        ((HEADS, 3, TOK, TOK), BF16),
        ((8, 2, 16, D_OUT), F32),
        ((HEADS, 8, 16, D_OUT), F32),
        ((HEADS, 8, 16, D_OUT), BF16),
        ((HEADS, 8, 16, D_OUT), BF16),
        ((KV_HEADS, 8, 16, D_OUT), BF16),
        ((KV_HEADS, 8, 16, D_OUT), BF16),
        ((6, 4, 16, D_OUT), BF16),
        ((6, 4, 16, D_OUT), BF16),
        ((8, 16, D_OUT), BF16),
        ((8, 16, D_OUT), BF16),
        ((16, D_OUT), BF16),
        ((16, D_OUT), BF16),
        ((16, D_OUT), F32),
        ((16, D_OUT), F32),
        ((KV_HEADS, 2, TOK, HD), BF16),
        ((KV_HEADS, 2, TOK, HD), BF16),
        ((KV_HEADS, 2, TOK, HD), BF16),
        ((KV_HEADS, 2, TOK, HD), BF16),
        ((KV_HEADS, 2, TOK, HD), F32),
        ((KV_HEADS, 2, TOK, HD), F32),
        ((3, 8, 128), jnp.int32),
    ]
    dq, dk, dv, dw, sq = pl.pallas_call(
        body,
        out_shape=(
            jax.ShapeDtypeStruct((TOK, 2048), BF16),
            jax.ShapeDtypeStruct((TOK, 1024), BF16),
            jax.ShapeDtypeStruct((TOK, 1024), BF16),
            jax.ShapeDtypeStruct((2, 16, D_OUT), F32),
            jax.ShapeDtypeStruct((8, HD), F32),
        ),
        in_specs=[pl.BlockSpec(memory_space=pltpu.SMEM)] + [vm] * 6,
        out_specs=[vm] * 5,
        scratch_shapes=[pltpu.VMEM(s, d) for s, d in scratch]
        + [pltpu.SemaphoreType.DMA((CHANNELS,)), pltpu.SemaphoreType.DMA((CHANNELS,))],
        compiler_params=pltpu.CompilerParams(
            collective_id=0, has_side_effects=True, vmem_limit_bytes=67043328
        ),
        name="band",
    )(
        seq_len,
        queries[0],
        keys[0],
        values[0],
        out_grad[0],
        out_weight.reshape(2, 16, D_OUT),
        jnp.full((8, 128), seq_len[0], jnp.int32),
    )
    entries = SLOTS * (HEADS + 2 * KV_HEADS) * HD + HEADS * HD * D_OUT
    grad_rms = jnp.sqrt(lax.psum(jnp.sum(sq), AXES) / entries)
    return dq[None], dk[None], dv[None], dw.reshape(32, D_OUT), grad_rms


def solution(mesh):
    split = Mesh(mesh.devices.reshape(4, 2, 8, 2, 2), AXES)
    rows = P(DP, SEQ, None)
    return jax.shard_map(
        shards,
        mesh=split,
        in_specs=(rows, rows, rows, rows, P(SEQ, None), P(DP)),
        out_specs=(rows, rows, rows, P(SEQ, None), P()),
        check_vma=False,
    )
```

```python
import jax
import jax.numpy as jnp
from jax import lax
from jax.experimental import pallas as pl
from jax.experimental.pallas import tpu as pltpu
from jax.sharding import Mesh
from jax.sharding import PartitionSpec as P

HEADS = 8
KV_HEADS = 4
GROUP = HEADS // KV_HEADS
HD = 256
D_OUT = 1792
WINDOW = 512
TOK = 256
SEQ = ("sy", "sx", "sz")
DP = ("dx", "dc")
AXES = ("sy", "sx", "sz", "dx", "dc")
N_DEV_SEQ = 64
SLOTS = 4 * 16384

SCALE = 0.0625
CAP = 50.0
LOG2E = 1.4426950408889634
CHANNELS = 144

F32 = jnp.float32
BF16 = jnp.bfloat16
MESH = pl.DeviceIdType.MESH


def dot_nt(a, b):
    return lax.dot_general(a, b, (((1,), (1,)), ((), ())), preferred_element_type=F32)


def dot_nn(a, b):
    return lax.dot_general(a, b, (((1,), (0,)), ((), ())), preferred_element_type=F32)


def dot_tn(a, b):
    return lax.dot_general(a, b, (((0,), (0,)), ((), ())), preferred_element_type=F32)


def col(n):
    return pl.ds(n * HD, HD)


def body(
    len_ref, q_ref, k_ref, v_ref, og_ref, w_ref, lt_ref,
    dq_ref, dk_ref, dv_ref, dw_ref, rms_ref,
    sq_ref, wf, k1, k2, v1, v2, mk, at, pb, pw, tw, dwm, sdb, rdb, xsb, xrb, ysb, yrb, zsb, zrb,
    fsb, frb, hsb, hrb, c2s, c2r, cms, cmr, c1, c0, lts, tz, ty, tx, ssem, rsem,
):
    y, xl, z, xh, c = (lax.axis_index(a) for a in AXES)
    oc = 1 - c
    pos = (y * 2 + xl) * 8 + z

    def at_seq(s):
        return (lax.div(s, 16), lax.rem(lax.div(s, 8), 2), lax.rem(s, 8), xh, c)

    def mod(a, n):
        return lax.rem(a, n)

    right = at_seq(mod(pos + 1, N_DEV_SEQ))
    left = at_seq(mod(pos + N_DEV_SEQ - 1, N_DEV_SEQ))
    yn = (mod(y + 1, 4), xl, z, xh, c)
    yp = (mod(y + 3, 4), xl, z, xh, c)
    xr = (y, 1 - xl, z, mod(xh + xl, 2), c)
    xp = (y, 1 - xl, z, mod(xh + 1 - xl, 2), c)
    x2 = (y, xl, z, 1 - xh, c)
    x2o = (y, xl, z, 1 - xh, oc)
    cp = (y, xl, z, xh, oc)

    def zpeer(k):
        return (y, xl, mod(z + k, 8), xh, c)

    ids = {}
    sent = {}

    def channel(name):
        return ids.setdefault(name, len(ids))

    def send(name, src, dst, dev):
        n = channel(name)
        d = pltpu.make_async_remote_copy(
            src_ref=src, dst_ref=dst, send_sem=ssem.at[n], recv_sem=rsem.at[n],
            device_id=dev, device_id_type=MESH,
        )
        d.start()
        sent[name] = (n, src)

    def recv(name, dst):
        n = channel(name)
        pltpu.make_async_remote_copy(
            src_ref=dst, dst_ref=dst, send_sem=ssem.at[n], recv_sem=rsem.at[n],
            device_id=cp, device_id_type=MESH,
        ).wait_recv()

    barrier = pltpu.get_barrier_semaphore()
    yo = (mod(y + 2, 4), xl, z, xh, c)
    xro = (*xr[:4], oc)
    xpo = (*xp[:4], oc)
    peers = [zpeer(k) for k in range(1, 8)]
    peers += [right, left, yn, yp, yo, xr, xp, xro, xpo, x2, x2o, cp]
    for dev in peers:
        pl.semaphore_signal(barrier, inc=1, device_id=dev, device_id_type=MESH)
    pl.semaphore_wait(barrier, len(peers))

    def unit(j):
        return mod(y + j, 4) * 2 + xl

    def other(j):
        return mod(y + j, 4) * 2 + 1 - xl

    def part(u, p, h):
        return wf.at[pl.ds(8 * u + 4 * p, 4), h]

    ours = [[[part(unit(j), p, h) for h in (c, oc)] for p in range(2)] for j in range(4)]

    first = 1 - lax.div(z + 7, 8)
    last = lax.div(z, 7)
    one_way = jnp.logical_and(z == 0, xl == 0)

    def x_dev(p, outer):
        near = mod(xh + xl, 2) if p == 0 else mod(xh + 1 - xl, 2)
        return (y, 1 - xl, z, outer * (1 - xh) + (1 - outer) * near, c)

    x_devs = [[x_dev(p, first if j in (1, 3) else 0) for p in range(2)] for j in range(4)]

    def spread(j, p):
        ref = ours[j][p][0]
        send(f"x{j}{p}", ref, ref, x_devs[j][p])
        send(f"d{j}{p}", ref, ref, cp)

    def gather_z():
        for k in (1, 7, 6, 2, 3, 5, 4):
            send(f"z{k}", w_ref.at[c], wf.at[pos - z + (9 - k) % 8, c], zpeer(k))
        wf[pos - z + 1, c] = w_ref[c]

    def gather_y(p):
        for k in ((1, 7, 6), (2, 3, 5, 4))[p]:
            recv(f"z{k}", wf.at[pos - z + (9 - k) % 8, c])
        ref = ours[0][p][0]

        @pl.when(jnp.logical_not(one_way))
        def _():
            send(f"ya{p}", ref, ref, yn)

        send(f"yb{p}", ref, ref, yp)
        spread(0, p)

    def gather_ya(p):
        ref = ours[3][p][0]
        recv(f"ya{p}", ref)
        if p == 0:

            @pl.when(jnp.logical_not(one_way))
            def _():
                send("yf0", ref, ref, yn)

        spread(3, p)

    def gather_yb(p):
        ref = ours[1][p][0]
        recv(f"yb{p}", ref)
        if p == 0:

            @pl.when(one_way)
            def _():
                send("yf0", ref, ref, yp)

        else:
            send("yf1", ref, ref, yp)
        spread(1, p)

    def gather_y0():
        @pl.when(jnp.logical_not(one_way))
        def _():
            gather_ya(0)

        gather_yb(0)

    def gather_y1():
        gather_yb(1)

        @pl.when(jnp.logical_not(one_way))
        def _():
            gather_ya(1)

    def gather_y2(p):
        ref = ours[2][p][0]
        recv(f"yf{p}", ref)

        @pl.when(one_way)
        def _():
            send(f"ya{p}", ref, ref, yp)

        spread(2, p)

    def gather_y3():
        @pl.when(one_way)
        def _():
            for p in range(2):
                gather_ya(p)

    def gather_x(j):
        for p in range(2):
            ref = part(other(j), p, c)
            recv(f"x{j}{p}", ref)
            send(f"e{j}{p}", ref, ref, cp)

    def gather_done():
        for j in range(4):
            for p in range(2):
                recv(f"d{j}{p}", ours[j][p][1])
                recv(f"e{j}{p}", part(other(j), p, oc))

    def unless_last(fn):
        pl.when(z != 7)(fn)

    def if_last(fn):
        pl.when(z == 7)(fn)

    def halo_own(kh):
        send(f"ok{kh}", k_ref.at[:, col(kh)], k1.at[:, col(kh)], right)
        send(f"ov{kh}", v_ref.at[:, col(kh)], v1.at[:, col(kh)], right)

    def halo_relay(kh):
        recv(f"ok{kh}", k1.at[:, col(kh)])
        send(f"fk{kh}", k1.at[:, col(kh)], k2.at[:, col(kh)], right)
        recv(f"ov{kh}", v1.at[:, col(kh)])
        send(f"fv{kh}", v1.at[:, col(kh)], v2.at[:, col(kh)], right)

    def halo_last(kh):
        recv(f"fk{kh}", k2.at[:, col(kh)])
        recv(f"fv{kh}", v2.at[:, col(kh)])

    def lengths_send():
        send("l0", lt_ref, lts.at[0], cp)
        send("l1", lt_ref, lts.at[1], x2)
        send("l2", lt_ref, lts.at[2], x2o)

    def lengths():
        for n in range(3):
            recv(f"l{n}", lts.at[n])
        total = (lt_ref[...] + lts[0] + lts[1] + lts[2]).astype(F32)[0:1, 0:1]
        return SLOTS / total, lax.rsqrt(total)

    def masked():
        row = lax.broadcasted_iota(jnp.int32, (TOK, 1), 0)
        mk[...] = jnp.where(row < len_ref[0] - pos * TOK, og_ref[...], jnp.zeros((), BF16))

    def forward(h):
        kh = h // GROUP
        q = q_ref[:, col(h)]
        row = lax.broadcasted_iota(jnp.int32, (TOK, TOK), 0)
        cl = lax.broadcasted_iota(jnp.int32, (TOK, TOK), 1)
        far = jnp.where(pos >= 2, 0, 2 * TOK)
        near = jnp.where(pos >= 1, 0, 2 * TOK)
        allowed = (cl - row > far, cl >= near, cl <= row)
        es, ws = [], []
        total = jnp.zeros((TOK, 1), F32)
        for b, ref in enumerate((k2, k1, k_ref)):
            t = jnp.tanh(dot_nt(q, ref[:, col(kh)]) * (SCALE / CAP))
            e = jnp.where(allowed[b], jnp.exp2(t * (CAP * LOG2E)), 0.0)
            total = total + jnp.sum(e, axis=1, keepdims=True)
            es.append(e)
            ws.append(e * (SCALE - SCALE * (t * t)))
        inv = 1.0 / total
        out = jnp.zeros((TOK, HD), F32)
        for b, ref in enumerate((v2, v1, v_ref)):
            p = (es[b] * inv).astype(BF16)
            pb[h, b] = p
            pw[h, b] = (ws[b] * inv).astype(BF16)
            out = out + dot_nn(p, ref[:, col(kh)])
        at[:, col(h)] = out.astype(BF16)

    def weight_part(h):
        tw[...] = dot_tn(at[:, col(h)], mk[...]).reshape(8, 2, 16, D_OUT)
        sdb[h] = tw[:, oc].astype(BF16)
        dwm[h] = tw[:, c]
        send(f"rd{h}", sdb.at[h], rdb.at[h], cp)

    def forward_pair(kh):
        for g in range(GROUP):
            forward(kh * GROUP + g)
            weight_part(kh * GROUP + g)

    def reduce_x(kh):
        for g in range(GROUP):
            h = kh * GROUP + g
            recv(f"rd{h}", rdb.at[h])
        outer = last if kh == 3 else first + last
        u, o = kh * 2 + xl, kh * 2 + 1 - xl
        xsb[kh] = (dwm[o] + rdb[o].astype(F32)).astype(BF16)
        dwm[u] = dwm[u] + rdb[u].astype(F32)
        for p in range(2):
            send(f"rx{kh}{p}", xsb.at[kh, pl.ds(4 * p, 4)], xrb.at[kh, pl.ds(4 * p, 4)], x_dev(p, outer))

    def reduce_x_done(kh):
        for p in range(2):
            recv(f"rx{kh}{p}", xrb.at[kh, pl.ds(4 * p, 4)])
        u = kh * 2 + xl
        dwm[u] = dwm[u] + xrb[kh].astype(F32)

    def mine(kh, p):
        return dwm[kh * 2 + xl, pl.ds(4 * p, 4)]

    y_refs = [ysb.at[n] for n in range(6)]

    def y_send(n, value, dev):
        ysb[n] = value.astype(BF16)
        send(f"r{n}", y_refs[n], yrb.at[n], dev)

    def role(kh, j):
        return pl.when(mod(kh - y + 4, 4) == j)

    def reduce_y(kh):
        @role(kh, 2)
        def _():
            y_send(0, mine(kh, 0), yn)
            y_send(1, mine(kh, 1), yp)

        @role(kh, 1)
        def _():
            y_send(2, mine(kh, 1), yn)

        @role(kh, 3)
        def _():
            y_send(3, mine(kh, 0), yp)

    def reduce_y2(kh):
        @role(kh, 1)
        def _():
            recv("r0", yrb.at[0])
            y_send(4, mine(kh, 0) + yrb[0].astype(F32), yn)

        @role(kh, 3)
        def _():
            recv("r1", yrb.at[1])
            y_send(5, mine(kh, 1) + yrb[1].astype(F32), yp)

    z_refs = [zsb.at[mod(z + k, 8)] for k in range(8)]

    def reduce_z(kh):
        @role(kh, 0)
        def _():
            for n in range(2, 6):
                recv(f"r{n}", yrb.at[n])
            u = kh * 2 + xl
            lo = mine(kh, 0) + yrb[3].astype(F32) + yrb[4].astype(F32)
            hi = mine(kh, 1) + yrb[2].astype(F32) + yrb[5].astype(F32)
            dwm[u, pl.ds(0, 4)] = lo
            dwm[u, pl.ds(4, 4)] = hi
            zsb[pl.ds(0, 4)] = lo.astype(BF16)
            zsb[pl.ds(4, 4)] = hi.astype(BF16)
            for k in range(1, 8):
                send(f"rz{k}", z_refs[k], zrb.at[k], zpeer(k))

    def reduce_dp():
        total = dwm[unit(0), z]
        for k in range(1, 8):
            recv(f"rz{k}", zrb.at[k])
            total = total + zrb[k].astype(F32)
        fsb[...] = total.astype(BF16)
        send("f", fsb, frb, x2)

    def reduce_swap(weight_scale):
        recv("f", frb)
        total = (fsb[...].astype(F32) + frb[...].astype(F32)) * weight_scale
        hsb[...] = total
        send("h", hsb, hrb, cp)
        dw_ref[c] = total
        square = total * total * 0.5
        acc = sq_ref[...]
        for n in range(D_OUT // HD):
            acc = acc + square[0:8, n * HD : (n + 1) * HD] + square[8:16, n * HD : (n + 1) * HD]
        sq_ref[...] = acc

    def reduce_end():
        recv("h", hrb)
        dw_ref[oc] = hrb[...]

    def squares(x):
        sq_ref[...] += jnp.sum((x * x).reshape(TOK // 8, 8, HD), axis=0)

    def backward(kh, act_scale):
        sk = [None] * 3
        sv = [None] * 3
        for g in range(GROUP):
            h = kh * GROUP + g
            q = q_ref[:, col(h)]
            blocks = [wf[8 * h + mod(n + 9 - z, 8)].reshape(32, D_OUT) for n in range(8)]
            wh = jnp.concatenate(blocks, axis=0)
            ga = dot_nt(mk[...], wh).astype(BF16)
            delta = jnp.sum(ga.astype(F32) * at[:, col(h)].astype(F32), axis=1, keepdims=True)
            dq = jnp.zeros((TOK, HD), F32)
            for b, (kr, vr) in enumerate(((k2, v2), (k1, v1), (k_ref, v_ref))):
                dp = dot_nt(ga, vr[:, col(kh)])
                ds = (pw[h, b].astype(F32) * (dp - delta)).astype(BF16)
                dq = dq + dot_nn(ds, kr[:, col(kh)])
                dk = dot_tn(ds, q)
                dv = dot_tn(pb[h, b], ga)
                sk[b] = dk if g == 0 else sk[b] + dk
                sv[b] = dv if g == 0 else sv[b] + dv
            dq = dq * act_scale
            squares(dq)
            dq_ref[:, col(h)] = dq.astype(BF16)
        c2s[kh, 0] = sk[0].astype(BF16)
        c2s[kh, 1] = sv[0].astype(BF16)
        send(f"b{kh}", c2s.at[kh], c2r.at[kh], left)
        c1[kh, 0] = sk[1]
        c1[kh, 1] = sv[1]
        c0[kh, 0] = sk[2]
        c0[kh, 1] = sv[2]

    def combine(kh):
        recv(f"b{kh}", c2r.at[kh])
        cms[kh] = (c1[kh] + c2r[kh].astype(F32)).astype(BF16)
        send(f"m{kh}", cms.at[kh], cmr.at[kh], left)

    def finish(kh, act_scale):
        recv(f"m{kh}", cmr.at[kh])
        for n, ref in enumerate((dk_ref, dv_ref)):
            total = (c0[kh, n] + cmr[kh, n].astype(F32)) * act_scale
            squares(total)
            ref[:, col(kh)] = total.astype(BF16)

    def everyone(name, buf, at_me, value, devs):
        buf[at_me] = value
        for n, dev in enumerate(devs):
            send(f"{name}{n}", buf.at[at_me], buf.at[at_me], dev)

    def heard(name, buf, slots):
        for n, slot in enumerate(slots):
            recv(f"{name}{n}", buf.at[slot])
        total = buf[0]
        for n in range(1, buf.shape[0]):
            total = total + buf[n]
        return total

    def rms():
        own = jnp.sum(jnp.sum(sq_ref[...], axis=0, keepdims=True), axis=1, keepdims=True)
        own = jnp.broadcast_to(own, (8, 128))
        everyone("sz", tz, z, own, [zpeer(k) for k in range(1, 8)])
        total = heard("sz", tz, [mod(z + 8 - k, 8) for k in range(1, 8)])
        everyone("sy", ty, y, total, [yn, yp, yo])
        total = heard("sy", ty, [mod(y + 3, 4), mod(y + 1, 4), mod(y + 2, 4)])
        x = xh * 2 + xl
        up, down, far = mod(x + 1, 4), mod(x + 3, 4), mod(x + 2, 4)
        everyone("sx", tx, x * 2 + c, total, [xr, xp, x2, xro, xpo, x2o, cp])
        slots = [down * 2 + c, up * 2 + c, far * 2 + c]
        slots += [down * 2 + oc, up * 2 + oc, far * 2 + oc, x * 2 + oc]
        total = heard("sx", tx, slots)
        entries = SLOTS * (HEADS + 2 * KV_HEADS) * HD + HEADS * HD * D_OUT
        rms_ref[...] = jnp.sqrt(total * (1.0 / entries))

    sq_ref[...] = jnp.zeros_like(sq_ref)
    with jax.named_scope("gather_z"):
        gather_z()
    with jax.named_scope("lengths_send"):
        lengths_send()
    with jax.named_scope("halo_own#0"):
        halo_own(0)
    with jax.named_scope("masked"):
        masked()
    with jax.named_scope("gather_y#0"):
        gather_y(0)
    with jax.named_scope("lengths"):
        act_scale, weight_scale = lengths()
    with jax.named_scope("gather_y#1"):
        gather_y(1)
    with jax.named_scope("gather_y0"):
        gather_y0()
    with jax.named_scope("halo_relay#0"):
        halo_relay(0)
    with jax.named_scope("halo_own#1"):
        unless_last(lambda: halo_own(1))
    with jax.named_scope("gather_y1"):
        gather_y1()
    with jax.named_scope("gather_y2#0"):
        gather_y2(0)
    with jax.named_scope("gather_y2#1"):
        gather_y2(1)
    with jax.named_scope("gather_y3"):
        gather_y3()
    with jax.named_scope("halo_last#0"):
        halo_last(0)
    with jax.named_scope("forward_pair#0"):
        forward_pair(0)
    with jax.named_scope("halo_relay#1"):
        pl.when(first + last == 0)(lambda: [halo_relay(1), halo_own(2)] and None)
        pl.when(first == 1)(lambda: halo_own(2))
    with jax.named_scope("gather_x#0"):
        gather_x(0)
    with jax.named_scope("gather_x#1"):
        gather_x(1)
    with jax.named_scope("gather_x#3"):
        gather_x(3)
    with jax.named_scope("gather_x#2"):
        gather_x(2)
    with jax.named_scope("reduce_x#0"):
        reduce_x(0)
    with jax.named_scope("gather_done"):
        gather_done()
    with jax.named_scope("halo_late#1"):
        if_last(lambda: [halo_own(1), halo_relay(1), halo_own(2)] and None)
    with jax.named_scope("backward#0"):
        backward(0, act_scale)
    with jax.named_scope("halo_late#0"):
        pl.when(first == 1)(lambda: halo_relay(1))
    with jax.named_scope("halo_relay#2"):
        halo_relay(2)
    with jax.named_scope("halo_own#3"):
        halo_own(3)
    with jax.named_scope("halo_last#1"):
        halo_last(1)
    with jax.named_scope("forward_pair#1"):
        forward_pair(1)
    with jax.named_scope("reduce_x_done#0"):
        reduce_x_done(0)
    with jax.named_scope("reduce_y#0"):
        reduce_y(0)
    with jax.named_scope("reduce_x#1"):
        reduce_x(1)
    with jax.named_scope("backward#1"):
        backward(1, act_scale)
    with jax.named_scope("combine#0"):
        combine(0)
    with jax.named_scope("halo_relay#3"):
        halo_relay(3)
    with jax.named_scope("halo_last#2"):
        halo_last(2)
    with jax.named_scope("forward_pair#2"):
        forward_pair(2)
    with jax.named_scope("reduce_y2#0"):
        reduce_y2(0)
    with jax.named_scope("reduce_x_done#1"):
        reduce_x_done(1)
    with jax.named_scope("reduce_y#1"):
        reduce_y(1)
    with jax.named_scope("reduce_x#2"):
        reduce_x(2)
    with jax.named_scope("backward#2"):
        backward(2, act_scale)
    with jax.named_scope("combine#1"):
        combine(1)
    with jax.named_scope("halo_last#3"):
        halo_last(3)
    with jax.named_scope("forward_pair#3"):
        forward_pair(3)
    with jax.named_scope("reduce_z#0"):
        reduce_z(0)
    with jax.named_scope("reduce_y2#1"):
        reduce_y2(1)
    with jax.named_scope("reduce_x_done#2"):
        reduce_x_done(2)
    with jax.named_scope("reduce_y#2"):
        reduce_y(2)
    with jax.named_scope("reduce_x#3"):
        reduce_x(3)
    with jax.named_scope("backward#3"):
        backward(3, act_scale)
    with jax.named_scope("combine#2"):
        combine(2)
    with jax.named_scope("finish#0"):
        finish(0, act_scale)
    with jax.named_scope("reduce_z#1"):
        reduce_z(1)
    with jax.named_scope("reduce_y2#2"):
        reduce_y2(2)
    with jax.named_scope("reduce_x_done#3"):
        reduce_x_done(3)
    with jax.named_scope("reduce_y#3"):
        reduce_y(3)
    with jax.named_scope("finish#1"):
        finish(1, act_scale)
    with jax.named_scope("reduce_z#2"):
        reduce_z(2)
    with jax.named_scope("combine#3"):
        combine(3)
    with jax.named_scope("reduce_y2#3"):
        reduce_y2(3)
    with jax.named_scope("finish#2"):
        finish(2, act_scale)
    with jax.named_scope("reduce_z#3"):
        reduce_z(3)
    with jax.named_scope("reduce_dp"):
        reduce_dp()
    with jax.named_scope("finish#3"):
        finish(3, act_scale)
    with jax.named_scope("reduce_swap"):
        reduce_swap(weight_scale)
    with jax.named_scope("rms"):
        rms()
    with jax.named_scope("reduce_end"):
        reduce_end()
    with jax.named_scope("drain"):
        for n, src in sent.values():
            pltpu.make_async_remote_copy(
                src_ref=src, dst_ref=src, send_sem=ssem.at[n], recv_sem=rsem.at[n],
                device_id=cp, device_id_type=MESH,
            ).wait_send()


def shards(queries, keys, values, out_grad, out_weight, seq_len):
    vm = pl.BlockSpec(memory_space=pltpu.VMEM)
    scratch = [
        ((8, HD), F32),
        ((64, 2, 16, D_OUT), BF16),
        ((TOK, 1024), BF16),
        ((TOK, 1024), BF16),
        ((TOK, 1024), BF16),
        ((TOK, 1024), BF16),
        ((TOK, D_OUT), BF16),
        ((TOK, 2048), BF16),
        ((HEADS, 3, TOK, TOK), BF16),
        ((HEADS, 3, TOK, TOK), BF16),
        ((8, 2, 16, D_OUT), F32),
        ((HEADS, 8, 16, D_OUT), F32),
        ((HEADS, 8, 16, D_OUT), BF16),
        ((HEADS, 8, 16, D_OUT), BF16),
        ((KV_HEADS, 8, 16, D_OUT), BF16),
        ((KV_HEADS, 8, 16, D_OUT), BF16),
        ((6, 4, 16, D_OUT), BF16),
        ((6, 4, 16, D_OUT), BF16),
        ((8, 16, D_OUT), BF16),
        ((8, 16, D_OUT), BF16),
        ((16, D_OUT), BF16),
        ((16, D_OUT), BF16),
        ((16, D_OUT), F32),
        ((16, D_OUT), F32),
        ((KV_HEADS, 2, TOK, HD), BF16),
        ((KV_HEADS, 2, TOK, HD), BF16),
        ((KV_HEADS, 2, TOK, HD), BF16),
        ((KV_HEADS, 2, TOK, HD), BF16),
        ((KV_HEADS, 2, TOK, HD), F32),
        ((KV_HEADS, 2, TOK, HD), F32),
        ((3, 8, 128), jnp.int32),
        ((8, 8, 128), F32),
        ((4, 8, 128), F32),
        ((8, 8, 128), F32),
    ]
    dq, dk, dv, dw, rms = pl.pallas_call(
        body,
        out_shape=(
            jax.ShapeDtypeStruct((TOK, 2048), BF16),
            jax.ShapeDtypeStruct((TOK, 1024), BF16),
            jax.ShapeDtypeStruct((TOK, 1024), BF16),
            jax.ShapeDtypeStruct((2, 16, D_OUT), F32),
            jax.ShapeDtypeStruct((8, 128), F32),
        ),
        in_specs=[pl.BlockSpec(memory_space=pltpu.SMEM)] + [vm] * 6,
        out_specs=[vm] * 5,
        scratch_shapes=[pltpu.VMEM(s, d) for s, d in scratch]
        + [pltpu.SemaphoreType.DMA((CHANNELS,)), pltpu.SemaphoreType.DMA((CHANNELS,))],
        compiler_params=pltpu.CompilerParams(
            collective_id=0, has_side_effects=True, vmem_limit_bytes=67043328
        ),
        name="band",
    )(
        seq_len,
        queries[0],
        keys[0],
        values[0],
        out_grad[0],
        out_weight.reshape(2, 16, D_OUT),
        jnp.full((8, 128), seq_len[0], jnp.int32),
    )
    return dq[None], dk[None], dv[None], dw.reshape(32, D_OUT), rms[0, 0]


def solution(mesh):
    split = Mesh(mesh.devices.reshape(4, 2, 8, 2, 2), AXES)
    rows = P(DP, SEQ, None)
    return jax.shard_map(
        shards,
        mesh=split,
        in_specs=(rows, rows, rows, rows, P(SEQ, None), P(DP)),
        out_specs=(rows, rows, rows, P(SEQ, None), P()),
        check_vma=False,
    )
```

```python
import jax
import jax.numpy as jnp
from jax import lax
from jax.experimental import pallas as pl
from jax.experimental.pallas import tpu as pltpu
from jax.sharding import Mesh
from jax.sharding import PartitionSpec as P

HEADS = 8
KV_HEADS = 4
GROUP = HEADS // KV_HEADS
HD = 256
D_OUT = 1792
WINDOW = 512
TOK = 256
SEQ = ("sy", "sx", "sz")
DP = ("dx", "dc")
AXES = ("sy", "sx", "sz", "dx", "dc")
N_DEV_SEQ = 64
SLOTS = 4 * 16384

SCALE = 0.0625
CAP = 50.0
LOG2E = 1.4426950408889634
CHANNELS = 144

F32 = jnp.float32
BF16 = jnp.bfloat16
MESH = pl.DeviceIdType.MESH


def dot_nt(a, b):
    return lax.dot_general(a, b, (((1,), (1,)), ((), ())), preferred_element_type=F32)


def dot_nn(a, b):
    return lax.dot_general(a, b, (((1,), (0,)), ((), ())), preferred_element_type=F32)


def dot_tn(a, b):
    return lax.dot_general(a, b, (((0,), (0,)), ((), ())), preferred_element_type=F32)


def col(n):
    return pl.ds(n * HD, HD)


def body(
    len_ref, q_ref, k_ref, v_ref, og_ref, w_ref, lt_ref,
    dq_ref, dk_ref, dv_ref, dw_ref, rms_ref,
    sq_ref, wf, k1, k2, v1, v2, mk, mk2, at, at2, ga, gs, pb, pw, tw, dwm, sdb, rdb, ysb, yrb, zsb, zrb,
    fsb, frb, hsb, hrb, c2s, c2r, cms, cmr, c1, c0, lts, tz, ty, tx, ssem, rsem,
):
    y, xl, z, xh, c = (lax.axis_index(a) for a in AXES)
    oc = 1 - c
    pos = (y * 2 + xl) * 8 + z

    def at_seq(s):
        return (lax.div(s, 16), lax.rem(lax.div(s, 8), 2), lax.rem(s, 8), xh, c)

    def mod(a, n):
        return lax.rem(a, n)

    right = at_seq(mod(pos + 1, N_DEV_SEQ))
    left = at_seq(mod(pos + N_DEV_SEQ - 1, N_DEV_SEQ))
    yn = (mod(y + 1, 4), xl, z, xh, c)
    yp = (mod(y + 3, 4), xl, z, xh, c)
    xr = (y, 1 - xl, z, mod(xh + xl, 2), c)
    xp = (y, 1 - xl, z, mod(xh + 1 - xl, 2), c)
    x2 = (y, xl, z, 1 - xh, c)
    x2o = (y, xl, z, 1 - xh, oc)
    cp = (y, xl, z, xh, oc)
    pair = (y, 1 - xl, z, 1 - xh, c)

    def zpeer(k):
        return (y, xl, mod(z + k, 8), xh, c)

    ids = {}
    sent = {}

    def channel(name):
        return ids.setdefault(name, len(ids))

    def send(name, src, dst, dev):
        n = channel(name)
        d = pltpu.make_async_remote_copy(
            src_ref=src, dst_ref=dst, send_sem=ssem.at[n], recv_sem=rsem.at[n],
            device_id=dev, device_id_type=MESH,
        )
        d.start()
        sent[name] = (n, src)

    def recv(name, dst):
        n = channel(name)
        pltpu.make_async_remote_copy(
            src_ref=dst, dst_ref=dst, send_sem=ssem.at[n], recv_sem=rsem.at[n],
            device_id=cp, device_id_type=MESH,
        ).wait_recv()

    barrier = pltpu.get_barrier_semaphore()
    yo = (mod(y + 2, 4), xl, z, xh, c)
    xro = (*xr[:4], oc)
    xpo = (*xp[:4], oc)
    peers = [zpeer(k) for k in range(1, 8)]
    peers += [right, left, yn, yp, yo, xr, xp, xro, xpo, x2, x2o, cp]
    for dev in peers:
        pl.semaphore_signal(barrier, inc=1, device_id=dev, device_id_type=MESH)
    pl.semaphore_wait(barrier, len(peers))

    def unit(j):
        return mod(y + j, 4)

    def part(u, p, h):
        return wf.at[pl.ds(8 * u + 4 * p, 4), h]

    ours = [[[part(unit(j), p, h) for h in (c, oc)] for p in range(2)] for j in range(4)]

    one_way = jnp.logical_and(z == 0, xl == 0)

    def spread(j, p):
        ref = ours[j][p][0]
        send(f"d{j}{p}", ref, ref, cp)

    def gather_z():
        for k in (1, 7, 6, 2, 3, 5, 4):
            send(f"z{k}", w_ref.at[c], wf.at[8 * y + (9 - k) % 8, c], zpeer(k))
        wf[8 * y + 1, c] = w_ref[c]

    def gather_y(p):
        for k in ((1, 7, 6), (2, 3, 5, 4))[p]:
            recv(f"z{k}", wf.at[8 * y + (9 - k) % 8, c])
        ref = ours[0][p][0]
        if p == 0:
            send("ya0", ref, ref, yn)
        else:

            @pl.when(jnp.logical_not(one_way))
            def _():
                send("ya1", ref, ref, yn)

        send(f"yb{p}", ref, ref, yp)
        spread(0, p)

    def gather_y0():
        ref = ours[3][0][0]
        recv("ya0", ref)

        @pl.when(jnp.logical_not(one_way))
        def _():
            send("yf0", ref, ref, yn)

        spread(3, 0)
        ref = ours[1][0][0]
        recv("yb0", ref)

        @pl.when(one_way)
        def _():
            send("yf0", ref, ref, yp)

        spread(1, 0)

    def gather_ya1():
        recv("ya1", ours[3][1][0])
        spread(3, 1)

    def gather_y1():
        ref = ours[1][1][0]
        recv("yb1", ref)
        send("yf1", ref, ref, yp)
        spread(1, 1)
        pl.when(jnp.logical_not(one_way))(gather_ya1)

    def gather_y2(p):
        ref = ours[2][p][0]
        recv(f"yf{p}", ref)
        if p == 1:

            @pl.when(one_way)
            def _():
                send("ya1", ref, ref, yp)

        spread(2, p)

    def gather_y3():
        pl.when(one_way)(gather_ya1)

    def halo_own(kh):
        send(f"ok{kh}", k_ref.at[:, col(kh)], k1.at[:, col(kh)], right)
        send(f"ov{kh}", v_ref.at[:, col(kh)], v1.at[:, col(kh)], right)

    def halo_relay(kh):
        recv(f"ok{kh}", k1.at[:, col(kh)])
        send(f"fk{kh}", k1.at[:, col(kh)], k2.at[:, col(kh)], right)
        recv(f"ov{kh}", v1.at[:, col(kh)])
        send(f"fv{kh}", v1.at[:, col(kh)], v2.at[:, col(kh)], right)

    def relay_a():
        pl.when(z < 7)(lambda: [halo_relay(0), halo_own(1)] and None)

    def relay_b():
        pl.when(z == 7)(lambda: [halo_relay(0), halo_own(1)] and None)

    def halo_last(kh):
        recv(f"fk{kh}", k2.at[:, col(kh)])
        recv(f"fv{kh}", v2.at[:, col(kh)])

    def lengths_send():
        send("l0", lt_ref, lts.at[0], cp)
        send("l1", lt_ref, lts.at[1], x2)
        send("l2", lt_ref, lts.at[2], x2o)

    def lengths():
        for n in range(3):
            recv(f"l{n}", lts.at[n])
        total = (lt_ref[...] + lts[0] + lts[1] + lts[2]).astype(F32)[0:1, 0:1]
        return SLOTS / total, lax.rsqrt(total)

    def masked():
        row = lax.broadcasted_iota(jnp.int32, (TOK, 1), 0)
        mk[...] = jnp.where(row < len_ref[0] - pos * TOK, og_ref[...], jnp.zeros((), BF16))
        send("xm", mk, mk2, pair)

    def forward(h):
        kh = h // GROUP
        q = q_ref[:, col(h)]
        row = lax.broadcasted_iota(jnp.int32, (TOK, TOK), 0)
        cl = lax.broadcasted_iota(jnp.int32, (TOK, TOK), 1)
        far = jnp.where(pos >= 2, 0, 2 * TOK)
        near = jnp.where(pos >= 1, 0, 2 * TOK)
        allowed = (cl - row > far, cl >= near, cl <= row)
        es, ws = [], []
        total = jnp.zeros((TOK, 1), F32)
        for b, ref in enumerate((k2, k1, k_ref)):
            t = jnp.tanh(dot_nt(q, ref[:, col(kh)]) * (SCALE / CAP))
            e = jnp.where(allowed[b], jnp.exp2(t * (CAP * LOG2E)), 0.0)
            total = total + jnp.sum(e, axis=1, keepdims=True)
            es.append(e)
            ws.append(e * (SCALE - SCALE * (t * t)))
        inv = 1.0 / total
        out = jnp.zeros((TOK, HD), F32)
        for b, ref in enumerate((v2, v1, v_ref)):
            p = (es[b] * inv).astype(BF16)
            pb[h, b] = p
            pw[h, b] = (ws[b] * inv).astype(BF16)
            out = out + dot_nn(p, ref[:, col(kh)])
        at[h] = out.astype(BF16)

    def forward_pair(kh):
        for g in range(GROUP):
            forward(kh * GROUP + g)
        send(f"xa{kh}", at.at[kh * GROUP + 1 - xl], at2.at[kh], pair)

    def project(kh):
        if kh == 0:
            recv("xm", mk2)
        for j in range(4):

            @pl.when(mod(kh - y + 4, 4) == j)
            def _():
                for p in range(2):
                    recv(f"d{j}{p}", ours[j][p][1])

        blocks = [wf[8 * kh + mod(n + 9 - z, 8)].reshape(32, D_OUT) for n in range(8)]
        wh = jnp.concatenate(blocks, axis=0)
        gs[kh] = dot_nt(mk2[...], wh).astype(BF16)
        send(f"xg{kh}", gs.at[kh], ga.at[kh, xl], pair)
        ga[kh, xl] = dot_nt(mk[...], wh).astype(BF16)

    def weight(kh):
        recv(f"xa{kh}", at2.at[kh])
        total = dot_tn(at[kh * GROUP + xl], mk[...]) + dot_tn(at2[kh], mk2[...])
        tw[...] = total.reshape(8, 2, 16, D_OUT)
        sdb[kh] = tw[:, oc].astype(BF16)
        dwm[kh] = tw[:, c]
        send(f"rd{kh}", sdb.at[kh], rdb.at[kh], cp)

    def mine(kh, p):
        return dwm[kh, pl.ds(4 * p, 4)]

    y_refs = [ysb.at[n] for n in range(6)]

    def y_send(n, value, dev):
        ysb[n] = value.astype(BF16)
        send(f"r{n}", y_refs[n], yrb.at[n], dev)

    def role(kh, j):
        return pl.when(mod(kh - y + 4, 4) == j)

    one = xl * lax.div(z, 7)

    def role_if(kh, j, flag):
        return pl.when(jnp.logical_and(mod(kh - y + 4, 4) == j, one == flag))

    def y_relay(n, kh, p):
        recv(f"r{n}", yrb.at[n])
        return mine(kh, p) + yrb[n].astype(F32)

    def reduce_y(kh):
        recv(f"rd{kh}", rdb.at[kh])
        dwm[kh] = dwm[kh] + rdb[kh].astype(F32)

        @role_if(kh, 2, 0)
        def _():
            y_send(0, mine(kh, 0), yn)
            y_send(1, mine(kh, 1), yp)

        @role_if(kh, 1, 0)
        def _():
            y_send(2, mine(kh, 1), yn)

        @role_if(kh, 3, 0)
        def _():
            y_send(3, mine(kh, 0), yp)

        @role_if(kh, 3, 1)
        def _():
            y_send(0, mine(kh, 0), yn)
            y_send(1, mine(kh, 1), yn)

    def reduce_y2(kh):
        @role_if(kh, 1, 0)
        def _():
            y_send(4, y_relay(0, kh, 0), yn)

        @role_if(kh, 3, 0)
        def _():
            y_send(5, y_relay(1, kh, 1), yp)

        @role_if(kh, 2, 1)
        def _():
            y_send(2, y_relay(0, kh, 0), yn)
            y_send(3, y_relay(1, kh, 1), yn)

    def reduce_y3(kh):
        @role_if(kh, 1, 1)
        def _():
            y_send(4, y_relay(2, kh, 0), yn)
            y_send(5, y_relay(3, kh, 1), yn)

    z_refs = [zsb.at[mod(z + k, 8)] for k in range(8)]

    def reduce_z(kh):
        @role_if(kh, 0, 0)
        def _():
            recv("r3", yrb.at[3])
            recv("r2", yrb.at[2])
            for p in range(2):
                rows = pl.ds(4 * p, 4)
                dwm[kh, rows] = mine(kh, p) + yrb[3 - p].astype(F32)

        @role(kh, 0)
        def _():
            for p in range(2):
                rows = pl.ds(4 * p, 4)
                total = y_relay(4 + p, kh, p)
                dwm[kh, rows] = total
                zsb[rows] = total.astype(BF16)
            for k in range(1, 8):
                send(f"rz{k}", z_refs[k], zrb.at[k], zpeer(k))

    def reduce_dp():
        total = dwm[y, z]
        for k in range(1, 8):
            recv(f"rz{k}", zrb.at[k])
            total = total + zrb[k].astype(F32)
        fsb[...] = total.astype(BF16)
        send("f", fsb, frb, x2)

    def reduce_swap(weight_scale):
        recv("f", frb)
        total = (fsb[...].astype(F32) + frb[...].astype(F32)) * weight_scale
        hsb[...] = total
        send("h", hsb, hrb, cp)
        dw_ref[c] = total
        square = total * total * 0.5
        acc = sq_ref[...]
        for n in range(D_OUT // HD):
            acc = acc + square[0:8, n * HD : (n + 1) * HD] + square[8:16, n * HD : (n + 1) * HD]
        sq_ref[...] = acc

    def reduce_end():
        recv("h", hrb)
        dw_ref[oc] = hrb[...]

    def squares(x):
        sq_ref[...] += jnp.sum((x * x).reshape(TOK // 8, 8, HD), axis=0)

    def backward(kh, act_scale):
        recv(f"xg{kh}", ga.at[kh, 1 - xl])
        sk = [None] * 3
        sv = [None] * 3
        for g in range(GROUP):
            h = kh * GROUP + g
            q = q_ref[:, col(h)]
            gh = ga[kh, g]
            delta = jnp.sum(gh.astype(F32) * at[h].astype(F32), axis=1, keepdims=True)
            dq = jnp.zeros((TOK, HD), F32)
            for b, (kr, vr) in enumerate(((k2, v2), (k1, v1), (k_ref, v_ref))):
                dp = dot_nt(gh, vr[:, col(kh)])
                ds = (pw[h, b].astype(F32) * (dp - delta)).astype(BF16)
                dq = dq + dot_nn(ds, kr[:, col(kh)])
                dk = dot_tn(ds, q)
                dv = dot_tn(pb[h, b], gh)
                sk[b] = dk if g == 0 else sk[b] + dk
                sv[b] = dv if g == 0 else sv[b] + dv
            dq = dq * act_scale
            squares(dq)
            dq_ref[:, col(h)] = dq.astype(BF16)
        c2s[kh, 0] = sk[0].astype(BF16)
        c2s[kh, 1] = sv[0].astype(BF16)
        send(f"b{kh}", c2s.at[kh], c2r.at[kh], left)
        c1[kh, 0] = sk[1]
        c1[kh, 1] = sv[1]
        c0[kh, 0] = sk[2]
        c0[kh, 1] = sv[2]

    def combine(kh):
        recv(f"b{kh}", c2r.at[kh])
        cms[kh] = (c1[kh] + c2r[kh].astype(F32)).astype(BF16)
        send(f"m{kh}", cms.at[kh], cmr.at[kh], left)

    def finish(kh, act_scale):
        recv(f"m{kh}", cmr.at[kh])
        for n, ref in enumerate((dk_ref, dv_ref)):
            total = (c0[kh, n] + cmr[kh, n].astype(F32)) * act_scale
            squares(total)
            ref[:, col(kh)] = total.astype(BF16)

    def everyone(name, buf, at_me, value, devs):
        buf[at_me] = value
        for n, dev in enumerate(devs):
            send(f"{name}{n}", buf.at[at_me], buf.at[at_me], dev)

    def heard(name, buf, slots):
        for n, slot in enumerate(slots):
            recv(f"{name}{n}", buf.at[slot])
        total = buf[0]
        for n in range(1, buf.shape[0]):
            total = total + buf[n]
        return total

    def rms():
        own = jnp.sum(jnp.sum(sq_ref[...], axis=0, keepdims=True), axis=1, keepdims=True)
        own = jnp.broadcast_to(own, (8, 128))
        everyone("sz", tz, z, own, [zpeer(k) for k in range(1, 8)])
        total = heard("sz", tz, [mod(z + 8 - k, 8) for k in range(1, 8)])
        everyone("sy", ty, y, total, [yn, yp, yo])
        total = heard("sy", ty, [mod(y + 3, 4), mod(y + 1, 4), mod(y + 2, 4)])
        x = xh * 2 + xl
        up, down, far = mod(x + 1, 4), mod(x + 3, 4), mod(x + 2, 4)
        everyone("sx", tx, x * 2 + c, total, [xr, xp, x2, xro, xpo, x2o, cp])
        slots = [down * 2 + c, up * 2 + c, far * 2 + c]
        slots += [down * 2 + oc, up * 2 + oc, far * 2 + oc, x * 2 + oc]
        total = heard("sx", tx, slots)
        entries = SLOTS * (HEADS + 2 * KV_HEADS) * HD + HEADS * HD * D_OUT
        rms_ref[...] = jnp.sqrt(total * (1.0 / entries))

    sq_ref[...] = jnp.zeros_like(sq_ref)
    with jax.named_scope("gather_z"):
        gather_z()
    with jax.named_scope("lengths_send"):
        lengths_send()
    with jax.named_scope("halo_own#0"):
        halo_own(0)
    with jax.named_scope("masked"):
        masked()
    with jax.named_scope("gather_y#0"):
        gather_y(0)
    with jax.named_scope("lengths"):
        act_scale, weight_scale = lengths()
    with jax.named_scope("gather_y#1"):
        gather_y(1)
    with jax.named_scope("gather_y0"):
        gather_y0()
    with jax.named_scope("relay_a"):
        relay_a()
    with jax.named_scope("gather_y1"):
        gather_y1()
    with jax.named_scope("gather_y2#0"):
        gather_y2(0)
    with jax.named_scope("relay_b"):
        relay_b()
    with jax.named_scope("gather_y2#1"):
        gather_y2(1)
    with jax.named_scope("halo_last#0"):
        halo_last(0)
    with jax.named_scope("forward_pair#0"):
        forward_pair(0)
    with jax.named_scope("halo_relay#1"):
        halo_relay(1)
    with jax.named_scope("halo_own#2"):
        halo_own(2)
    with jax.named_scope("gather_y3"):
        gather_y3()
    with jax.named_scope("project#0"):
        project(0)
    with jax.named_scope("project#1"):
        project(1)
    with jax.named_scope("weight#0"):
        weight(0)
    with jax.named_scope("project#2"):
        project(2)
    with jax.named_scope("project#3"):
        project(3)
    with jax.named_scope("backward#0"):
        backward(0, act_scale)
    with jax.named_scope("halo_relay#2"):
        halo_relay(2)
    with jax.named_scope("halo_own#3"):
        halo_own(3)
    with jax.named_scope("halo_last#1"):
        halo_last(1)
    with jax.named_scope("forward_pair#1"):
        forward_pair(1)
    with jax.named_scope("reduce_y#0"):
        reduce_y(0)
    with jax.named_scope("backward#1"):
        backward(1, act_scale)
    with jax.named_scope("weight#1"):
        weight(1)
    with jax.named_scope("combine#0"):
        combine(0)
    with jax.named_scope("halo_relay#3"):
        halo_relay(3)
    with jax.named_scope("halo_last#2"):
        halo_last(2)
    with jax.named_scope("forward_pair#2"):
        forward_pair(2)
    with jax.named_scope("backward#2"):
        backward(2, act_scale)
    with jax.named_scope("reduce_y2#0"):
        reduce_y2(0)
    with jax.named_scope("reduce_y#1"):
        reduce_y(1)
    with jax.named_scope("weight#2"):
        weight(2)
    with jax.named_scope("halo_last#3"):
        halo_last(3)
    with jax.named_scope("forward_pair#3"):
        forward_pair(3)
    with jax.named_scope("combine#1"):
        combine(1)
    with jax.named_scope("backward#3"):
        backward(3, act_scale)
    with jax.named_scope("reduce_y2#1"):
        reduce_y2(1)
    with jax.named_scope("reduce_y#2"):
        reduce_y(2)
    with jax.named_scope("weight#3"):
        weight(3)
    with jax.named_scope("reduce_y3#0"):
        reduce_y3(0)
    with jax.named_scope("combine#2"):
        combine(2)
    with jax.named_scope("reduce_y#3"):
        reduce_y(3)
    with jax.named_scope("reduce_y2#2"):
        reduce_y2(2)
    with jax.named_scope("reduce_y3#1"):
        reduce_y3(1)
    with jax.named_scope("combine#3"):
        combine(3)
    with jax.named_scope("reduce_y2#3"):
        reduce_y2(3)
    with jax.named_scope("reduce_y3#2"):
        reduce_y3(2)
    with jax.named_scope("finish#0"):
        finish(0, act_scale)
    with jax.named_scope("reduce_y3#3"):
        reduce_y3(3)
    with jax.named_scope("reduce_z#0"):
        reduce_z(0)
    with jax.named_scope("reduce_z#1"):
        reduce_z(1)
    with jax.named_scope("reduce_z#2"):
        reduce_z(2)
    with jax.named_scope("reduce_z#3"):
        reduce_z(3)
    with jax.named_scope("finish#1"):
        finish(1, act_scale)
    with jax.named_scope("finish#2"):
        finish(2, act_scale)
    with jax.named_scope("reduce_dp"):
        reduce_dp()
    with jax.named_scope("finish#3"):
        finish(3, act_scale)
    with jax.named_scope("reduce_swap"):
        reduce_swap(weight_scale)
    with jax.named_scope("rms"):
        rms()
    with jax.named_scope("reduce_end"):
        reduce_end()
    with jax.named_scope("drain"):
        for n, src in sent.values():
            pltpu.make_async_remote_copy(
                src_ref=src, dst_ref=src, send_sem=ssem.at[n], recv_sem=rsem.at[n],
                device_id=cp, device_id_type=MESH,
            ).wait_send()


def shards(queries, keys, values, out_grad, out_weight, seq_len):
    vm = pl.BlockSpec(memory_space=pltpu.VMEM)
    scratch = [
        ((8, HD), F32),
        ((32, 2, 16, D_OUT), BF16),
        ((TOK, 1024), BF16),
        ((TOK, 1024), BF16),
        ((TOK, 1024), BF16),
        ((TOK, 1024), BF16),
        ((TOK, D_OUT), BF16),
        ((TOK, D_OUT), BF16),
        ((HEADS, TOK, HD), BF16),
        ((KV_HEADS, TOK, HD), BF16),
        ((KV_HEADS, 2, TOK, HD), BF16),
        ((KV_HEADS, TOK, HD), BF16),
        ((HEADS, 3, TOK, TOK), BF16),
        ((HEADS, 3, TOK, TOK), BF16),
        ((8, 2, 16, D_OUT), F32),
        ((KV_HEADS, 8, 16, D_OUT), F32),
        ((KV_HEADS, 8, 16, D_OUT), BF16),
        ((KV_HEADS, 8, 16, D_OUT), BF16),
        ((6, 4, 16, D_OUT), BF16),
        ((6, 4, 16, D_OUT), BF16),
        ((8, 16, D_OUT), BF16),
        ((8, 16, D_OUT), BF16),
        ((16, D_OUT), BF16),
        ((16, D_OUT), BF16),
        ((16, D_OUT), F32),
        ((16, D_OUT), F32),
        ((KV_HEADS, 2, TOK, HD), BF16),
        ((KV_HEADS, 2, TOK, HD), BF16),
        ((KV_HEADS, 2, TOK, HD), BF16),
        ((KV_HEADS, 2, TOK, HD), BF16),
        ((KV_HEADS, 2, TOK, HD), F32),
        ((KV_HEADS, 2, TOK, HD), F32),
        ((3, 8, 128), jnp.int32),
        ((8, 8, 128), F32),
        ((4, 8, 128), F32),
        ((8, 8, 128), F32),
    ]
    dq, dk, dv, dw, rms = pl.pallas_call(
        body,
        out_shape=(
            jax.ShapeDtypeStruct((TOK, 2048), BF16),
            jax.ShapeDtypeStruct((TOK, 1024), BF16),
            jax.ShapeDtypeStruct((TOK, 1024), BF16),
            jax.ShapeDtypeStruct((2, 16, D_OUT), F32),
            jax.ShapeDtypeStruct((8, 128), F32),
        ),
        in_specs=[pl.BlockSpec(memory_space=pltpu.SMEM)] + [vm] * 6,
        out_specs=[vm] * 5,
        scratch_shapes=[pltpu.VMEM(s, d) for s, d in scratch]
        + [pltpu.SemaphoreType.DMA((CHANNELS,)), pltpu.SemaphoreType.DMA((CHANNELS,))],
        compiler_params=pltpu.CompilerParams(
            collective_id=0, has_side_effects=True, vmem_limit_bytes=67043328
        ),
        name="band",
    )(
        seq_len,
        queries[0],
        keys[0],
        values[0],
        out_grad[0],
        out_weight.reshape(2, 16, D_OUT),
        jnp.full((8, 128), seq_len[0], jnp.int32),
    )
    return dq[None], dk[None], dv[None], dw.reshape(32, D_OUT), rms[0, 0]


def solution(mesh):
    split = Mesh(mesh.devices.reshape(4, 2, 8, 2, 2), AXES)
    rows = P(DP, SEQ, None)
    return jax.shard_map(
        shards,
        mesh=split,
        in_specs=(rows, rows, rows, rows, P(SEQ, None), P(DP)),
        out_specs=(rows, rows, rows, P(SEQ, None), P()),
        check_vma=False,
    )
```

```python
import jax
import jax.numpy as jnp
from jax import lax
from jax.experimental import pallas as pl
from jax.experimental.pallas import tpu as pltpu
from jax.sharding import Mesh
from jax.sharding import PartitionSpec as P

HEADS = 8
KV_HEADS = 4
GROUP = HEADS // KV_HEADS
HD = 256
D_OUT = 1792
WINDOW = 512
TOK = 256
SEQ = ("sy", "sx", "sz")
DP = ("dx", "dc")
AXES = ("sy", "sx", "sz", "dx", "dc")
N_DEV_SEQ = 64
SLOTS = 4 * 16384

SCALE = 0.0625
CAP = 50.0
LOG2E = 1.4426950408889634
CHANNELS = 144

F32 = jnp.float32
BF16 = jnp.bfloat16
MESH = pl.DeviceIdType.MESH


def dot_nt(a, b):
    return lax.dot_general(a, b, (((1,), (1,)), ((), ())), preferred_element_type=F32)


def dot_nn(a, b):
    return lax.dot_general(a, b, (((1,), (0,)), ((), ())), preferred_element_type=F32)


def dot_tn(a, b):
    return lax.dot_general(a, b, (((0,), (0,)), ((), ())), preferred_element_type=F32)


def col(n):
    return pl.ds(n * HD, HD)


def body(
    len_ref, q_ref, k_ref, v_ref, og_ref, w_ref, lt_ref,
    dq_ref, dk_ref, dv_ref, dw_ref, rms_ref,
    sq_ref, wf, k1, k2, v1, v2, mk, mk2, at, at2, ga, gs, pb, pw, tw, dwm, sdb, rdb, ysb, yrb, zsb, zrb,
    fsb, frb, hsb, hrb, c2s, c2r, cms, cmr, c1, c0, lts, tz, ty, tx, ssem, rsem,
):
    y, xl, z, xh, c = (lax.axis_index(a) for a in AXES)
    oc = 1 - c
    pos = (y * 2 + xl) * 8 + z

    def at_seq(s):
        return (lax.div(s, 16), lax.rem(lax.div(s, 8), 2), lax.rem(s, 8), xh, c)

    def mod(a, n):
        return lax.rem(a, n)

    right = at_seq(mod(pos + 1, N_DEV_SEQ))
    left = at_seq(mod(pos + N_DEV_SEQ - 1, N_DEV_SEQ))
    yn = (mod(y + 1, 4), xl, z, xh, c)
    yp = (mod(y + 3, 4), xl, z, xh, c)
    xr = (y, 1 - xl, z, mod(xh + xl, 2), c)
    xp = (y, 1 - xl, z, mod(xh + 1 - xl, 2), c)
    x2 = (y, xl, z, 1 - xh, c)
    x2o = (y, xl, z, 1 - xh, oc)
    cp = (y, xl, z, xh, oc)
    pair = (y, 1 - xl, z, 1 - xh, c)

    def zpeer(k):
        return (y, xl, mod(z + k, 8), xh, c)

    ids = {}
    sent = {}

    def channel(name):
        return ids.setdefault(name, len(ids))

    def send(name, src, dst, dev):
        n = channel(name)
        d = pltpu.make_async_remote_copy(
            src_ref=src, dst_ref=dst, send_sem=ssem.at[n], recv_sem=rsem.at[n],
            device_id=dev, device_id_type=MESH,
        )
        d.start()
        sent[name] = (n, src)

    def recv(name, dst):
        n = channel(name)
        pltpu.make_async_remote_copy(
            src_ref=dst, dst_ref=dst, send_sem=ssem.at[n], recv_sem=rsem.at[n],
            device_id=cp, device_id_type=MESH,
        ).wait_recv()

    barrier = pltpu.get_barrier_semaphore()
    yo = (mod(y + 2, 4), xl, z, xh, c)
    xro = (*xr[:4], oc)
    xpo = (*xp[:4], oc)
    peers = [zpeer(k) for k in range(1, 8)]
    peers += [right, left, yn, yp, yo, xr, xp, xro, xpo, x2, x2o, cp]
    for dev in peers:
        pl.semaphore_signal(barrier, inc=1, device_id=dev, device_id_type=MESH)
    pl.semaphore_wait(barrier, len(peers))

    def unit(j):
        return mod(y + j, 4)

    def part(u, p, h):
        return wf.at[pl.ds(8 * u + 4 * p, 4), h]

    ours = [[[part(unit(j), p, h) for h in (c, oc)] for p in range(2)] for j in range(4)]

    one_way = jnp.logical_and(z == 0, xl == 0)

    def spread(j, p):
        ref = ours[j][p][0]
        send(f"d{j}{p}", ref, ref, cp)

    def gather_z():
        for k in (1, 7, 6, 2, 3, 5, 4):
            send(f"z{k}", w_ref.at[c], wf.at[8 * y + (9 - k) % 8, c], zpeer(k))
        wf[8 * y + 1, c] = w_ref[c]

    def gather_y(p):
        for k in ((1, 7, 6), (2, 3, 5, 4))[p]:
            recv(f"z{k}", wf.at[8 * y + (9 - k) % 8, c])
        ref = ours[0][p][0]
        if p == 0:
            send("ya0", ref, ref, yn)
        else:

            @pl.when(jnp.logical_not(one_way))
            def _():
                send("ya1", ref, ref, yn)

        send(f"yb{p}", ref, ref, yp)
        spread(0, p)

    def gather_y0():
        ref = ours[3][0][0]
        recv("ya0", ref)

        @pl.when(jnp.logical_not(one_way))
        def _():
            send("yf0", ref, ref, yn)

        spread(3, 0)
        ref = ours[1][0][0]
        recv("yb0", ref)

        @pl.when(one_way)
        def _():
            send("yf0", ref, ref, yp)

        spread(1, 0)

    def gather_ya1():
        recv("ya1", ours[3][1][0])
        spread(3, 1)

    def gather_y1():
        ref = ours[1][1][0]
        recv("yb1", ref)
        send("yf1", ref, ref, yp)
        spread(1, 1)
        pl.when(jnp.logical_not(one_way))(gather_ya1)

    def gather_y2(p):
        ref = ours[2][p][0]
        recv(f"yf{p}", ref)
        if p == 1:

            @pl.when(one_way)
            def _():
                send("ya1", ref, ref, yp)

        spread(2, p)

    def gather_y3():
        pl.when(one_way)(gather_ya1)

    def halo_own(kh):
        send(f"ok{kh}", k_ref.at[:, col(kh)], k1.at[:, col(kh)], right)
        send(f"ov{kh}", v_ref.at[:, col(kh)], v1.at[:, col(kh)], right)

    def halo_relay(kh):
        recv(f"ok{kh}", k1.at[:, col(kh)])
        send(f"fk{kh}", k1.at[:, col(kh)], k2.at[:, col(kh)], right)
        recv(f"ov{kh}", v1.at[:, col(kh)])
        send(f"fv{kh}", v1.at[:, col(kh)], v2.at[:, col(kh)], right)

    holds = xl * lax.div(z, 7)

    def relay_a():
        pl.when(z == 0)(lambda: [halo_own(1), halo_relay(0), halo_own(2)] and None)
        pl.when((holds == 0) & (z > 0))(lambda: [halo_relay(0), halo_own(1)] and None)

    def relay_b():
        pl.when(holds == 1)(lambda: [halo_relay(0), halo_own(1)] and None)

    def relay_c():
        pl.when(z == 0)(lambda: halo_own(3))
        pl.when(z > 0)(lambda: [halo_relay(1), halo_own(2)] and None)

    def relay_d():
        pl.when(z == 0)(lambda: halo_relay(1))

    def relay_e():
        halo_relay(2)
        pl.when(z > 0)(lambda: halo_own(3))

    def halo_last(kh):
        recv(f"fk{kh}", k2.at[:, col(kh)])
        recv(f"fv{kh}", v2.at[:, col(kh)])

    def lengths_send():
        send("l0", lt_ref, lts.at[0], cp)
        send("l1", lt_ref, lts.at[1], x2)
        send("l2", lt_ref, lts.at[2], x2o)

    def lengths():
        for n in range(3):
            recv(f"l{n}", lts.at[n])
        total = (lt_ref[...] + lts[0] + lts[1] + lts[2]).astype(F32)[0:1, 0:1]
        return SLOTS / total, lax.rsqrt(total)

    def masked():
        row = lax.broadcasted_iota(jnp.int32, (TOK, 1), 0)
        mk[...] = jnp.where(row < len_ref[0] - pos * TOK, og_ref[...], jnp.zeros((), BF16))
        send("xm", mk, mk2, pair)

    def forward(h):
        kh = h // GROUP
        q = q_ref[:, col(h)]
        row = lax.broadcasted_iota(jnp.int32, (TOK, TOK), 0)
        cl = lax.broadcasted_iota(jnp.int32, (TOK, TOK), 1)
        far = jnp.where(pos >= 2, 0, 2 * TOK)
        near = jnp.where(pos >= 1, 0, 2 * TOK)
        allowed = (cl - row > far, cl >= near, cl <= row)
        es, ws = [], []
        total = jnp.zeros((TOK, 1), F32)
        for b, ref in enumerate((k2, k1, k_ref)):
            t = jnp.tanh(dot_nt(q, ref[:, col(kh)]) * (SCALE / CAP))
            e = jnp.where(allowed[b], jnp.exp2(t * (CAP * LOG2E)), 0.0)
            total = total + jnp.sum(e, axis=1, keepdims=True)
            es.append(e)
            ws.append(e * (SCALE - SCALE * (t * t)))
        inv = 1.0 / total
        out = jnp.zeros((TOK, HD), F32)
        for b, ref in enumerate((v2, v1, v_ref)):
            p = (es[b] * inv).astype(BF16)
            pb[h, b] = p
            pw[h, b] = (ws[b] * inv).astype(BF16)
            out = out + dot_nn(p, ref[:, col(kh)])
        at[h] = out.astype(BF16)

    def forward_pair(kh):
        for g in range(GROUP):
            forward(kh * GROUP + g)
        send(f"xa{kh}", at.at[kh * GROUP + 1 - xl], at2.at[kh], pair)

    def project(kh):
        if kh == 0:
            recv("xm", mk2)
        for j in range(4):

            @pl.when(mod(kh - y + 4, 4) == j)
            def _():
                for p in range(2):
                    recv(f"d{j}{p}", ours[j][p][1])

        blocks = [wf[8 * kh + mod(n + 9 - z, 8)].reshape(32, D_OUT) for n in range(8)]
        wh = jnp.concatenate(blocks, axis=0)
        gs[kh] = dot_nt(mk2[...], wh).astype(BF16)
        send(f"xg{kh}", gs.at[kh], ga.at[kh, xl], pair)
        ga[kh, xl] = dot_nt(mk[...], wh).astype(BF16)

    def weight(kh):
        recv(f"xa{kh}", at2.at[kh])
        total = dot_tn(at[kh * GROUP + xl], mk[...]) + dot_tn(at2[kh], mk2[...])
        tw[...] = total.reshape(8, 2, 16, D_OUT)
        sdb[kh] = tw[:, oc].astype(BF16)
        dwm[kh] = tw[:, c]
        send(f"rd{kh}", sdb.at[kh], rdb.at[kh], cp)

    def mine(kh, p):
        return dwm[kh, pl.ds(4 * p, 4)]

    y_refs = [ysb.at[n] for n in range(6)]

    def y_send(n, value, dev):
        ysb[n] = value.astype(BF16)
        send(f"r{n}", y_refs[n], yrb.at[n], dev)

    def role(kh, j):
        return pl.when(mod(kh - y + 4, 4) == j)

    one = xl * lax.div(z, 7)

    def role_if(kh, j, flag):
        return pl.when(jnp.logical_and(mod(kh - y + 4, 4) == j, one == flag))

    def y_relay(n, kh, p):
        recv(f"r{n}", yrb.at[n])
        return mine(kh, p) + yrb[n].astype(F32)

    def reduce_y(kh):
        recv(f"rd{kh}", rdb.at[kh])
        dwm[kh] = dwm[kh] + rdb[kh].astype(F32)

        @role_if(kh, 2, 0)
        def _():
            y_send(0, mine(kh, 0), yn)
            y_send(1, mine(kh, 1), yp)

        @role_if(kh, 1, 0)
        def _():
            y_send(2, mine(kh, 1), yn)

        @role_if(kh, 3, 0)
        def _():
            y_send(3, mine(kh, 0), yp)

        @role_if(kh, 3, 1)
        def _():
            y_send(0, mine(kh, 0), yn)
            y_send(1, mine(kh, 1), yn)

    def reduce_y2(kh):
        @role_if(kh, 1, 0)
        def _():
            y_send(4, y_relay(0, kh, 0), yn)

        @role_if(kh, 3, 0)
        def _():
            y_send(5, y_relay(1, kh, 1), yp)

        @role_if(kh, 2, 1)
        def _():
            y_send(2, y_relay(0, kh, 0), yn)
            y_send(3, y_relay(1, kh, 1), yn)

    def reduce_y3(kh):
        @role_if(kh, 1, 1)
        def _():
            y_send(4, y_relay(2, kh, 0), yn)
            y_send(5, y_relay(3, kh, 1), yn)

    z_refs = [zsb.at[mod(z + k, 8)] for k in range(8)]

    def reduce_z(kh):
        @role_if(kh, 0, 0)
        def _():
            recv("r3", yrb.at[3])
            recv("r2", yrb.at[2])
            for p in range(2):
                rows = pl.ds(4 * p, 4)
                dwm[kh, rows] = mine(kh, p) + yrb[3 - p].astype(F32)

        for p in range(2):
            rows = pl.ds(4 * p, 4)

            @role(kh, 0)
            def _():
                total = y_relay(4 + p, kh, p)
                dwm[kh, rows] = total
                zsb[rows] = total.astype(BF16)

            for k in range(1, 8):

                @pl.when(jnp.logical_and(kh == y, lax.div(mod(z + k, 8), 4) == p))
                def _():
                    send(f"rz{k}", z_refs[k], zrb.at[k], zpeer(k))

    def reduce_dp():
        total = dwm[y, z]
        for k in range(1, 8):
            recv(f"rz{k}", zrb.at[k])
            total = total + zrb[k].astype(F32)
        fsb[...] = total.astype(BF16)
        send("f", fsb, frb, x2)

    def reduce_swap(weight_scale):
        recv("f", frb)
        total = (fsb[...].astype(F32) + frb[...].astype(F32)) * weight_scale
        hsb[...] = total
        send("h", hsb, hrb, cp)
        dw_ref[c] = total
        square = total * total * 0.5
        acc = sq_ref[...]
        for n in range(D_OUT // HD):
            acc = acc + square[0:8, n * HD : (n + 1) * HD] + square[8:16, n * HD : (n + 1) * HD]
        sq_ref[...] = acc

    def reduce_end():
        recv("h", hrb)
        dw_ref[oc] = hrb[...]

    def squares(x):
        sq_ref[...] += jnp.sum((x * x).reshape(TOK // 8, 8, HD), axis=0)

    def backward(kh, act_scale):
        recv(f"xg{kh}", ga.at[kh, 1 - xl])
        sk = [None] * 3
        sv = [None] * 3
        for g in range(GROUP):
            h = kh * GROUP + g
            q = q_ref[:, col(h)]
            gh = ga[kh, g]
            delta = jnp.sum(gh.astype(F32) * at[h].astype(F32), axis=1, keepdims=True)
            dq = jnp.zeros((TOK, HD), F32)
            for b, (kr, vr) in enumerate(((k2, v2), (k1, v1), (k_ref, v_ref))):
                dp = dot_nt(gh, vr[:, col(kh)])
                ds = (pw[h, b].astype(F32) * (dp - delta)).astype(BF16)
                dq = dq + dot_nn(ds, kr[:, col(kh)])
                dk = dot_tn(ds, q)
                dv = dot_tn(pb[h, b], gh)
                sk[b] = dk if g == 0 else sk[b] + dk
                sv[b] = dv if g == 0 else sv[b] + dv
            dq = dq * act_scale
            squares(dq)
            dq_ref[:, col(h)] = dq.astype(BF16)
        c2s[kh, 0] = sk[0].astype(BF16)
        c2s[kh, 1] = sv[0].astype(BF16)
        send(f"b{kh}", c2s.at[kh], c2r.at[kh], left)
        c1[kh, 0] = sk[1]
        c1[kh, 1] = sv[1]
        c0[kh, 0] = sk[2]
        c0[kh, 1] = sv[2]

    def combine(kh):
        recv(f"b{kh}", c2r.at[kh])
        cms[kh] = (c1[kh] + c2r[kh].astype(F32)).astype(BF16)
        send(f"m{kh}", cms.at[kh], cmr.at[kh], left)

    def finish(kh, act_scale):
        recv(f"m{kh}", cmr.at[kh])
        for n, ref in enumerate((dk_ref, dv_ref)):
            total = (c0[kh, n] + cmr[kh, n].astype(F32)) * act_scale
            squares(total)
            ref[:, col(kh)] = total.astype(BF16)

    def everyone(name, buf, at_me, value, devs):
        buf[at_me] = value
        for n, dev in enumerate(devs):
            send(f"{name}{n}", buf.at[at_me], buf.at[at_me], dev)

    def heard(name, buf, slots):
        for n, slot in enumerate(slots):
            recv(f"{name}{n}", buf.at[slot])
        total = buf[0]
        for n in range(1, buf.shape[0]):
            total = total + buf[n]
        return total

    def rms():
        own = jnp.sum(jnp.sum(sq_ref[...], axis=0, keepdims=True), axis=1, keepdims=True)
        own = jnp.broadcast_to(own, (8, 128))
        everyone("sz", tz, z, own, [zpeer(k) for k in range(1, 8)])
        total = heard("sz", tz, [mod(z + 8 - k, 8) for k in range(1, 8)])
        everyone("sy", ty, y, total, [yn, yp, yo])
        total = heard("sy", ty, [mod(y + 3, 4), mod(y + 1, 4), mod(y + 2, 4)])
        x = xh * 2 + xl
        up, down, far = mod(x + 1, 4), mod(x + 3, 4), mod(x + 2, 4)
        everyone("sx", tx, x * 2 + c, total, [xr, xp, x2, xro, xpo, x2o, cp])
        slots = [down * 2 + c, up * 2 + c, far * 2 + c]
        slots += [down * 2 + oc, up * 2 + oc, far * 2 + oc, x * 2 + oc]
        total = heard("sx", tx, slots)
        entries = SLOTS * (HEADS + 2 * KV_HEADS) * HD + HEADS * HD * D_OUT
        rms_ref[...] = jnp.sqrt(total * (1.0 / entries))

    sq_ref[...] = jnp.zeros_like(sq_ref)
    with jax.named_scope("gather_z"):
        gather_z()
    with jax.named_scope("lengths_send"):
        lengths_send()
    with jax.named_scope("halo_own#0"):
        halo_own(0)
    with jax.named_scope("masked"):
        masked()
    with jax.named_scope("gather_y#0"):
        gather_y(0)
    with jax.named_scope("lengths"):
        act_scale, weight_scale = lengths()
    with jax.named_scope("gather_y#1"):
        gather_y(1)
    with jax.named_scope("gather_y0"):
        gather_y0()
    with jax.named_scope("relay_a"):
        relay_a()
    with jax.named_scope("gather_y1"):
        gather_y1()
    with jax.named_scope("relay_b"):
        relay_b()
    with jax.named_scope("gather_y2#0"):
        gather_y2(0)
    with jax.named_scope("gather_y2#1"):
        gather_y2(1)
    with jax.named_scope("halo_last#0"):
        halo_last(0)
    with jax.named_scope("forward_pair#0"):
        forward_pair(0)
    with jax.named_scope("relay_c"):
        relay_c()
    with jax.named_scope("gather_y3"):
        gather_y3()
    with jax.named_scope("project#0"):
        project(0)
    with jax.named_scope("project#1"):
        project(1)
    with jax.named_scope("relay_d"):
        relay_d()
    with jax.named_scope("weight#0"):
        weight(0)
    with jax.named_scope("project#2"):
        project(2)
    with jax.named_scope("project#3"):
        project(3)
    with jax.named_scope("backward#0"):
        backward(0, act_scale)
    with jax.named_scope("relay_e"):
        relay_e()
    with jax.named_scope("halo_last#1"):
        halo_last(1)
    with jax.named_scope("forward_pair#1"):
        forward_pair(1)
    with jax.named_scope("reduce_y#0"):
        reduce_y(0)
    with jax.named_scope("backward#1"):
        backward(1, act_scale)
    with jax.named_scope("weight#1"):
        weight(1)
    with jax.named_scope("combine#0"):
        combine(0)
    with jax.named_scope("halo_relay#3"):
        halo_relay(3)
    with jax.named_scope("halo_last#2"):
        halo_last(2)
    with jax.named_scope("forward_pair#2"):
        forward_pair(2)
    with jax.named_scope("backward#2"):
        backward(2, act_scale)
    with jax.named_scope("reduce_y2#0"):
        reduce_y2(0)
    with jax.named_scope("reduce_y#1"):
        reduce_y(1)
    with jax.named_scope("halo_last#3"):
        halo_last(3)
    with jax.named_scope("forward_pair#3"):
        forward_pair(3)
    with jax.named_scope("weight#2"):
        weight(2)
    with jax.named_scope("backward#3"):
        backward(3, act_scale)
    with jax.named_scope("combine#1"):
        combine(1)
    with jax.named_scope("weight#3"):
        weight(3)
    with jax.named_scope("reduce_y#2"):
        reduce_y(2)
    with jax.named_scope("reduce_y#3"):
        reduce_y(3)
    with jax.named_scope("reduce_y2#1"):
        reduce_y2(1)
    with jax.named_scope("combine#2"):
        combine(2)
    with jax.named_scope("reduce_y3#0"):
        reduce_y3(0)
    with jax.named_scope("reduce_y2#2"):
        reduce_y2(2)
    with jax.named_scope("reduce_y3#1"):
        reduce_y3(1)
    with jax.named_scope("reduce_y2#3"):
        reduce_y2(3)
    with jax.named_scope("reduce_y3#2"):
        reduce_y3(2)
    with jax.named_scope("combine#3"):
        combine(3)
    with jax.named_scope("reduce_y3#3"):
        reduce_y3(3)
    with jax.named_scope("reduce_z#0"):
        reduce_z(0)
    with jax.named_scope("reduce_z#1"):
        reduce_z(1)
    with jax.named_scope("reduce_z#2"):
        reduce_z(2)
    with jax.named_scope("reduce_z#3"):
        reduce_z(3)
    with jax.named_scope("finish#0"):
        finish(0, act_scale)
    with jax.named_scope("finish#1"):
        finish(1, act_scale)
    with jax.named_scope("finish#2"):
        finish(2, act_scale)
    with jax.named_scope("reduce_dp"):
        reduce_dp()
    with jax.named_scope("finish#3"):
        finish(3, act_scale)
    with jax.named_scope("reduce_swap"):
        reduce_swap(weight_scale)
    with jax.named_scope("rms"):
        rms()
    with jax.named_scope("reduce_end"):
        reduce_end()
    with jax.named_scope("drain"):
        for n, src in sent.values():
            pltpu.make_async_remote_copy(
                src_ref=src, dst_ref=src, send_sem=ssem.at[n], recv_sem=rsem.at[n],
                device_id=cp, device_id_type=MESH,
            ).wait_send()


def publish(*refs):
    given, results, held, sem_in, sem_out = refs[:5], refs[5:10], refs[10:14], refs[14], refs[15]
    loads = [pltpu.make_async_copy(given[n], held[n], sem_in.at[n]) for n in range(4)]
    stores = [pltpu.make_async_copy(held[n], results[n], sem_out.at[n]) for n in range(4)]
    for load in loads:
        load.start()
    results[4][0, 0] = given[4][0, 0]
    for load, store in zip(loads, stores):
        load.wait()
        store.start()
    for store in stores:
        store.wait()


def shards(queries, keys, values, out_grad, out_weight, seq_len):
    vm = pl.BlockSpec(memory_space=pltpu.VMEM)
    scratch = [
        ((8, HD), F32),
        ((32, 2, 16, D_OUT), BF16),
        ((TOK, 1024), BF16),
        ((TOK, 1024), BF16),
        ((TOK, 1024), BF16),
        ((TOK, 1024), BF16),
        ((TOK, D_OUT), BF16),
        ((TOK, D_OUT), BF16),
        ((HEADS, TOK, HD), BF16),
        ((KV_HEADS, TOK, HD), BF16),
        ((KV_HEADS, 2, TOK, HD), BF16),
        ((KV_HEADS, TOK, HD), BF16),
        ((HEADS, 3, TOK, TOK), BF16),
        ((HEADS, 3, TOK, TOK), BF16),
        ((8, 2, 16, D_OUT), F32),
        ((KV_HEADS, 8, 16, D_OUT), F32),
        ((KV_HEADS, 8, 16, D_OUT), BF16),
        ((KV_HEADS, 8, 16, D_OUT), BF16),
        ((6, 4, 16, D_OUT), BF16),
        ((6, 4, 16, D_OUT), BF16),
        ((8, 16, D_OUT), BF16),
        ((8, 16, D_OUT), BF16),
        ((16, D_OUT), BF16),
        ((16, D_OUT), BF16),
        ((16, D_OUT), F32),
        ((16, D_OUT), F32),
        ((KV_HEADS, 2, TOK, HD), BF16),
        ((KV_HEADS, 2, TOK, HD), BF16),
        ((KV_HEADS, 2, TOK, HD), BF16),
        ((KV_HEADS, 2, TOK, HD), BF16),
        ((KV_HEADS, 2, TOK, HD), F32),
        ((KV_HEADS, 2, TOK, HD), F32),
        ((3, 8, 128), jnp.int32),
        ((8, 8, 128), F32),
        ((4, 8, 128), F32),
        ((8, 8, 128), F32),
    ]
    dq, dk, dv, dw, rms = pl.pallas_call(
        body,
        out_shape=(
            jax.ShapeDtypeStruct((TOK, 2048), BF16),
            jax.ShapeDtypeStruct((TOK, 1024), BF16),
            jax.ShapeDtypeStruct((TOK, 1024), BF16),
            jax.ShapeDtypeStruct((2, 16, D_OUT), F32),
            jax.ShapeDtypeStruct((8, 128), F32),
        ),
        in_specs=[pl.BlockSpec(memory_space=pltpu.SMEM)] + [vm] * 6,
        out_specs=[vm] * 5,
        scratch_shapes=[pltpu.VMEM(s, d) for s, d in scratch]
        + [pltpu.SemaphoreType.DMA((CHANNELS,)), pltpu.SemaphoreType.DMA((CHANNELS,))],
        compiler_params=pltpu.CompilerParams(
            collective_id=0, has_side_effects=True, vmem_limit_bytes=54 * 2**20
        ),
        name="band",
    )(
        seq_len,
        queries[0],
        keys[0],
        values[0],
        out_grad[0],
        out_weight.reshape(2, 16, D_OUT),
        jnp.full((8, 128), seq_len[0], jnp.int32),
    )
    shapes = [((TOK, 2048), BF16), ((TOK, 1024), BF16), ((TOK, 1024), BF16), ((32, D_OUT), F32)]
    anywhere = pl.BlockSpec(memory_space=pl.ANY)
    scalar = pl.BlockSpec(memory_space=pltpu.SMEM)
    dq, dk, dv, dw, rms = pl.pallas_call(
        publish,
        out_shape=[jax.ShapeDtypeStruct(a, d) for a, d in shapes + [((1, 1), F32)]],
        in_specs=[anywhere] * 4 + [scalar],
        out_specs=[anywhere] * 4 + [scalar],
        scratch_shapes=[pltpu.VMEM(a, d) for a, d in shapes]
        + [pltpu.SemaphoreType.DMA((4,)), pltpu.SemaphoreType.DMA((4,))],
        name="publish",
    )(dq, dk, dv, dw.reshape(32, D_OUT), rms)
    return dq[None], dk[None], dv[None], dw, rms.reshape(())


def solution(mesh):
    split = Mesh(mesh.devices.reshape(4, 2, 8, 2, 2), AXES)
    rows = P(DP, SEQ, None)
    return jax.shard_map(
        shards,
        mesh=split,
        in_specs=(rows, rows, rows, rows, P(SEQ, None), P(DP)),
        out_specs=(rows, rows, rows, P(SEQ, None), P()),
        check_vma=False,
    )
```

```python
import jax
import jax.numpy as jnp
from jax import lax
from jax.experimental import pallas as pl
from jax.experimental.pallas import tpu as pltpu
from jax.sharding import Mesh
from jax.sharding import PartitionSpec as P

HEADS = 8
KV_HEADS = 4
GROUP = HEADS // KV_HEADS
HD = 256
D_OUT = 1792
WINDOW = 512
TOK = 256
SEQ = ("sy", "sx", "sz")
DP = ("dx", "dc")
AXES = ("sy", "sx", "sz", "dx", "dc")
N_DEV_SEQ = 64
SLOTS = 4 * 16384

SCALE = 0.0625
CAP = 50.0
LOG2E = 1.4426950408889634
CHANNELS = 160
OFFSETS = [(a, b, d) for a in range(4) for b in range(4) for d in range(2) if a + b + d > 0]

F32 = jnp.float32
BF16 = jnp.bfloat16
MESH = pl.DeviceIdType.MESH


def dot_nt(a, b):
    return lax.dot_general(a, b, (((1,), (1,)), ((), ())), preferred_element_type=F32)


def dot_nn(a, b):
    return lax.dot_general(a, b, (((1,), (0,)), ((), ())), preferred_element_type=F32)


def dot_tn(a, b):
    return lax.dot_general(a, b, (((0,), (0,)), ((), ())), preferred_element_type=F32)


def col(n):
    return pl.ds(n * HD, HD)


def body(
    len_ref, q_ref, k_ref, v_ref, og_ref, w_ref, lt_ref,
    dq_ref, dk_ref, dv_ref, dw_ref, rms_ref,
    sq_ref, wf, k1, k2, v1, v2, mk, mk2, at, at2, ga, gs, pb, pw, tw, dwm, sdb, rdb, ysb, yrb, zsb, zrb,
    fsb, frb, hsb, hrb, c2s, c2r, cms, cmr, c1, c0, lts, tz, tp, ssem, rsem,
):
    y, xl, z, xh, c = (lax.axis_index(a) for a in AXES)
    oc = 1 - c
    pos = (y * 2 + xl) * 8 + z

    def at_seq(s):
        return (lax.div(s, 16), lax.rem(lax.div(s, 8), 2), lax.rem(s, 8), xh, c)

    def mod(a, n):
        return lax.rem(a, n)

    right = at_seq(mod(pos + 1, N_DEV_SEQ))
    left = at_seq(mod(pos + N_DEV_SEQ - 1, N_DEV_SEQ))
    yn = (mod(y + 1, 4), xl, z, xh, c)
    yp = (mod(y + 3, 4), xl, z, xh, c)
    xr = (y, 1 - xl, z, mod(xh + xl, 2), c)
    xp = (y, 1 - xl, z, mod(xh + 1 - xl, 2), c)
    x2 = (y, xl, z, 1 - xh, c)
    x2o = (y, xl, z, 1 - xh, oc)
    cp = (y, xl, z, xh, oc)
    pair = (y, 1 - xl, z, 1 - xh, c)

    def zpeer(k):
        return (y, xl, mod(z + k, 8), xh, c)

    ids = {}
    sent = {}

    def channel(name):
        return ids.setdefault(name, len(ids))

    def send(name, src, dst, dev):
        n = channel(name)
        d = pltpu.make_async_remote_copy(
            src_ref=src, dst_ref=dst, send_sem=ssem.at[n], recv_sem=rsem.at[n],
            device_id=dev, device_id_type=MESH,
        )
        d.start()
        sent[name] = (n, src)

    def recv(name, dst):
        n = channel(name)
        pltpu.make_async_remote_copy(
            src_ref=dst, dst_ref=dst, send_sem=ssem.at[n], recv_sem=rsem.at[n],
            device_id=cp, device_id_type=MESH,
        ).wait_recv()

    barrier = pltpu.get_barrier_semaphore()
    x = xh * 2 + xl

    def plane(dy, dx, dc):
        there = mod(x + dx, 4)
        return (mod(y + dy, 4), mod(there, 2), z, lax.div(there, 2), mod(c + dc, 2))

    def plane_slot(dy, dx, dc):
        return (mod(y + dy + 4, 4) * 4 + mod(x + dx + 4, 4)) * 2 + mod(c + dc, 2)

    peers = [zpeer(k) for k in range(1, 8)] + [plane(*o) for o in OFFSETS] + [right, left]
    for dev in peers:
        pl.semaphore_signal(barrier, inc=1, device_id=dev, device_id_type=MESH)
    pl.semaphore_wait(barrier, len(peers))

    def unit(j):
        return mod(y + j, 4)

    def part(u, p, h):
        return wf.at[pl.ds(8 * u + 4 * p, 4), h]

    ours = [[[part(unit(j), p, h) for h in (c, oc)] for p in range(2)] for j in range(4)]

    one_way = jnp.logical_and(z == 0, xl == 0)

    def spread(j, p):
        ref = ours[j][p][0]
        send(f"d{j}{p}", ref, ref, cp)

    def gather_z():
        for k in (1, 7, 6, 2, 3, 5, 4):
            send(f"z{k}", w_ref.at[c], wf.at[8 * y + (9 - k) % 8, c], zpeer(k))
        wf[8 * y + 1, c] = w_ref[c]

    def gather_y(p):
        for k in ((1, 7, 6), (2, 3, 5, 4))[p]:
            recv(f"z{k}", wf.at[8 * y + (9 - k) % 8, c])
        ref = ours[0][p][0]
        if p == 0:
            send("ya0", ref, ref, yn)
        else:

            @pl.when(jnp.logical_not(one_way))
            def _():
                send("ya1", ref, ref, yn)

        send(f"yb{p}", ref, ref, yp)
        spread(0, p)

    def gather_y0():
        ref = ours[3][0][0]
        recv("ya0", ref)

        @pl.when(jnp.logical_not(one_way))
        def _():
            send("yf0", ref, ref, yn)

        spread(3, 0)
        ref = ours[1][0][0]
        recv("yb0", ref)

        @pl.when(one_way)
        def _():
            send("yf0", ref, ref, yp)

        spread(1, 0)

    def gather_ya1():
        recv("ya1", ours[3][1][0])
        spread(3, 1)

    def gather_y1():
        ref = ours[1][1][0]
        recv("yb1", ref)
        send("yf1", ref, ref, yp)
        spread(1, 1)
        pl.when(jnp.logical_not(one_way))(gather_ya1)

    def gather_y2(p):
        ref = ours[2][p][0]
        recv(f"yf{p}", ref)
        if p == 1:

            @pl.when(one_way)
            def _():
                send("ya1", ref, ref, yp)

        spread(2, p)

    def gather_y3():
        pl.when(one_way)(gather_ya1)

    def halo_own(kh):
        send(f"ok{kh}", k_ref.at[:, col(kh)], k1.at[:, col(kh)], right)
        send(f"ov{kh}", v_ref.at[:, col(kh)], v1.at[:, col(kh)], right)

    def halo_relay(kh):
        recv(f"ok{kh}", k1.at[:, col(kh)])
        send(f"fk{kh}", k1.at[:, col(kh)], k2.at[:, col(kh)], right)
        recv(f"ov{kh}", v1.at[:, col(kh)])
        send(f"fv{kh}", v1.at[:, col(kh)], v2.at[:, col(kh)], right)

    holds = xl * lax.div(z, 7)

    def relay_a():
        pl.when(z == 0)(lambda: [halo_own(1), halo_relay(0), halo_own(2)] and None)
        pl.when((holds == 0) & (z > 0))(lambda: [halo_relay(0), halo_own(1)] and None)

    def relay_b():
        pl.when(holds == 1)(lambda: [halo_relay(0), halo_own(1)] and None)

    def relay_c():
        pl.when(z == 0)(lambda: halo_own(3))
        pl.when(z > 0)(lambda: [halo_relay(1), halo_own(2)] and None)

    def relay_d():
        pl.when(z == 0)(lambda: halo_relay(1))

    def relay_e():
        halo_relay(2)
        pl.when(z > 0)(lambda: halo_own(3))

    def halo_last(kh):
        recv(f"fk{kh}", k2.at[:, col(kh)])
        recv(f"fv{kh}", v2.at[:, col(kh)])

    def lengths_send():
        send("l0", lt_ref, lts.at[0], cp)
        send("l1", lt_ref, lts.at[1], x2)
        send("l2", lt_ref, lts.at[2], x2o)

    def lengths():
        for n in range(3):
            recv(f"l{n}", lts.at[n])
        total = (lt_ref[...] + lts[0] + lts[1] + lts[2]).astype(F32)[0:1, 0:1]
        return SLOTS / total, lax.rsqrt(total)

    def masked():
        row = lax.broadcasted_iota(jnp.int32, (TOK, 1), 0)
        mk[...] = jnp.where(row < len_ref[0] - pos * TOK, og_ref[...], jnp.zeros((), BF16))
        send("xm", mk, mk2, pair)

    def forward(h):
        kh = h // GROUP
        q = q_ref[:, col(h)]
        row = lax.broadcasted_iota(jnp.int32, (TOK, TOK), 0)
        cl = lax.broadcasted_iota(jnp.int32, (TOK, TOK), 1)
        far = jnp.where(pos >= 2, 0, 2 * TOK)
        near = jnp.where(pos >= 1, 0, 2 * TOK)
        allowed = (cl - row > far, cl >= near, cl <= row)
        es, ws = [], []
        total = jnp.zeros((TOK, 1), F32)
        for b, ref in enumerate((k2, k1, k_ref)):
            t = jnp.tanh(dot_nt(q, ref[:, col(kh)]) * (SCALE / CAP))
            e = jnp.where(allowed[b], jnp.exp2(t * (CAP * LOG2E)), 0.0)
            total = total + jnp.sum(e, axis=1, keepdims=True)
            es.append(e)
            ws.append(e * (SCALE - SCALE * (t * t)))
        inv = 1.0 / total
        out = jnp.zeros((TOK, HD), F32)
        for b, ref in enumerate((v2, v1, v_ref)):
            p = (es[b] * inv).astype(BF16)
            pb[h, b] = p
            pw[h, b] = (ws[b] * inv).astype(BF16)
            out = out + dot_nn(p, ref[:, col(kh)])
        at[h] = out.astype(BF16)

    def forward_pair(kh):
        for g in range(GROUP):
            forward(kh * GROUP + g)
        send(f"xa{kh}", at.at[kh * GROUP + 1 - xl], at2.at[kh], pair)

    def project(kh):
        if kh == 0:
            recv("xm", mk2)
        for j in range(4):

            @pl.when(mod(kh - y + 4, 4) == j)
            def _():
                for p in range(2):
                    recv(f"d{j}{p}", ours[j][p][1])

        blocks = [wf[8 * kh + mod(n + 9 - z, 8)].reshape(32, D_OUT) for n in range(8)]
        wh = jnp.concatenate(blocks, axis=0)
        gs[kh] = dot_nt(mk2[...], wh).astype(BF16)
        send(f"xg{kh}", gs.at[kh], ga.at[kh, xl], pair)
        ga[kh, xl] = dot_nt(mk[...], wh).astype(BF16)

    def weight(kh):
        recv(f"xa{kh}", at2.at[kh])
        total = dot_tn(at[kh * GROUP + xl], mk[...]) + dot_tn(at2[kh], mk2[...])
        tw[...] = total.reshape(8, 2, 16, D_OUT)
        sdb[kh] = tw[:, oc].astype(BF16)
        dwm[kh] = tw[:, c]
        send(f"rd{kh}", sdb.at[kh], rdb.at[kh], cp)

    def mine(kh, p):
        return dwm[kh, pl.ds(4 * p, 4)]

    y_refs = [ysb.at[n] for n in range(6)]

    def y_send(n, value, dev):
        ysb[n] = value.astype(BF16)
        send(f"r{n}", y_refs[n], yrb.at[n], dev)

    def role(kh, j):
        return pl.when(mod(kh - y + 4, 4) == j)

    one = xl * lax.div(z, 7)

    def role_if(kh, j, flag):
        return pl.when(jnp.logical_and(mod(kh - y + 4, 4) == j, one == flag))

    def y_relay(n, kh, p):
        recv(f"r{n}", yrb.at[n])
        return mine(kh, p) + yrb[n].astype(F32)

    def reduce_y(kh):
        recv(f"rd{kh}", rdb.at[kh])
        dwm[kh] = dwm[kh] + rdb[kh].astype(F32)

        @role_if(kh, 2, 0)
        def _():
            y_send(0, mine(kh, 0), yn)
            y_send(1, mine(kh, 1), yp)

        @role_if(kh, 1, 0)
        def _():
            y_send(2, mine(kh, 1), yn)

        @role_if(kh, 3, 0)
        def _():
            y_send(3, mine(kh, 0), yp)

        @role_if(kh, 3, 1)
        def _():
            y_send(0, mine(kh, 0), yn)
            y_send(1, mine(kh, 1), yn)

    def reduce_y2(kh):
        @role_if(kh, 1, 0)
        def _():
            y_send(4, y_relay(0, kh, 0), yn)

        @role_if(kh, 3, 0)
        def _():
            y_send(5, y_relay(1, kh, 1), yp)

        @role_if(kh, 2, 1)
        def _():
            y_send(2, y_relay(0, kh, 0), yn)
            y_send(3, y_relay(1, kh, 1), yn)

    def reduce_y3(kh):
        @role_if(kh, 1, 1)
        def _():
            y_send(4, y_relay(2, kh, 0), yn)
            y_send(5, y_relay(3, kh, 1), yn)

    z_refs = [zsb.at[mod(z + k, 8)] for k in range(8)]

    def reduce_z(kh):
        @role_if(kh, 0, 0)
        def _():
            recv("r3", yrb.at[3])
            recv("r2", yrb.at[2])
            for p in range(2):
                rows = pl.ds(4 * p, 4)
                dwm[kh, rows] = mine(kh, p) + yrb[3 - p].astype(F32)

        for p in range(2):
            rows = pl.ds(4 * p, 4)

            @role(kh, 0)
            def _():
                total = y_relay(4 + p, kh, p)
                dwm[kh, rows] = total
                zsb[rows] = total.astype(BF16)

            for k in range(1, 8):

                @pl.when(jnp.logical_and(kh == y, lax.div(mod(z + k, 8), 4) == p))
                def _():
                    send(f"rz{k}", z_refs[k], zrb.at[k], zpeer(k))

    def reduce_dp():
        total = dwm[y, z]
        for k in range(1, 8):
            recv(f"rz{k}", zrb.at[k])
            total = total + zrb[k].astype(F32)
        fsb[...] = total.astype(BF16)
        send("f", fsb, frb, x2)

    def reduce_swap(weight_scale):
        recv("f", frb)
        total = (fsb[...].astype(F32) + frb[...].astype(F32)) * weight_scale
        hsb[...] = total
        send("h", hsb, hrb, cp)
        dw_ref[c] = total
        square = total * total * 0.5
        acc = sq_ref[...]
        for n in range(D_OUT // HD):
            acc = acc + square[0:8, n * HD : (n + 1) * HD] + square[8:16, n * HD : (n + 1) * HD]
        sq_ref[...] = acc

    def reduce_end():
        recv("h", hrb)
        dw_ref[oc] = hrb[...]

    def squares(x):
        sq_ref[...] += jnp.sum((x * x).reshape(TOK // 8, 8, HD), axis=0)

    def backward(kh, act_scale):
        recv(f"xg{kh}", ga.at[kh, 1 - xl])
        sk = [None] * 3
        sv = [None] * 3
        for g in range(GROUP):
            h = kh * GROUP + g
            q = q_ref[:, col(h)]
            gh = ga[kh, g]
            delta = jnp.sum(gh.astype(F32) * at[h].astype(F32), axis=1, keepdims=True)
            dq = jnp.zeros((TOK, HD), F32)
            for b, (kr, vr) in enumerate(((k2, v2), (k1, v1), (k_ref, v_ref))):
                dp = dot_nt(gh, vr[:, col(kh)])
                ds = (pw[h, b].astype(F32) * (dp - delta)).astype(BF16)
                dq = dq + dot_nn(ds, kr[:, col(kh)])
                dk = dot_tn(ds, q)
                dv = dot_tn(pb[h, b], gh)
                sk[b] = dk if g == 0 else sk[b] + dk
                sv[b] = dv if g == 0 else sv[b] + dv
            dq = dq * act_scale
            squares(dq)
            dq_ref[:, col(h)] = dq.astype(BF16)
        c2s[kh, 0] = sk[0].astype(BF16)
        c2s[kh, 1] = sv[0].astype(BF16)
        send(f"b{kh}", c2s.at[kh], c2r.at[kh], left)
        c1[kh, 0] = sk[1]
        c1[kh, 1] = sv[1]
        c0[kh, 0] = sk[2]
        c0[kh, 1] = sv[2]

    def combine(kh):
        recv(f"b{kh}", c2r.at[kh])
        cms[kh] = (c1[kh] + c2r[kh].astype(F32)).astype(BF16)
        send(f"m{kh}", cms.at[kh], cmr.at[kh], left)

    def finish(kh, act_scale):
        recv(f"m{kh}", cmr.at[kh])
        for n, ref in enumerate((dk_ref, dv_ref)):
            total = (c0[kh, n] + cmr[kh, n].astype(F32)) * act_scale
            squares(total)
            ref[:, col(kh)] = total.astype(BF16)

    def everyone(name, buf, at_me, value, devs):
        buf[at_me] = value
        for n, dev in enumerate(devs):
            send(f"{name}{n}", buf.at[at_me], buf.at[at_me], dev)

    def heard(name, buf, slots):
        for n, slot in enumerate(slots):
            recv(f"{name}{n}", buf.at[slot])
        total = buf[0]
        for n in range(1, buf.shape[0]):
            total = total + buf[n]
        return total

    def rms():
        own = jnp.sum(jnp.sum(sq_ref[...], axis=0, keepdims=True), axis=1, keepdims=True)
        own = jnp.broadcast_to(own, (8, 128))
        everyone("sz", tz, z, own, [zpeer(k) for k in range(1, 8)])
        total = heard("sz", tz, [mod(z + 8 - k, 8) for k in range(1, 8)])
        everyone("sp", tp, plane_slot(0, 0, 0), total, [plane(*o) for o in OFFSETS])
        total = heard("sp", tp, [plane_slot(-dy, -dx, dc) for dy, dx, dc in OFFSETS])
        entries = SLOTS * (HEADS + 2 * KV_HEADS) * HD + HEADS * HD * D_OUT
        rms_ref[0, 0] = jnp.sqrt(total * (1.0 / entries))[0, 0]

    sq_ref[...] = jnp.zeros_like(sq_ref)
    with jax.named_scope("gather_z"):
        gather_z()
    with jax.named_scope("lengths_send"):
        lengths_send()
    with jax.named_scope("halo_own#0"):
        halo_own(0)
    with jax.named_scope("masked"):
        masked()
    with jax.named_scope("gather_y#0"):
        gather_y(0)
    with jax.named_scope("lengths"):
        act_scale, weight_scale = lengths()
    with jax.named_scope("gather_y#1"):
        gather_y(1)
    with jax.named_scope("gather_y0"):
        gather_y0()
    with jax.named_scope("relay_a"):
        relay_a()
    with jax.named_scope("gather_y1"):
        gather_y1()
    with jax.named_scope("relay_b"):
        relay_b()
    with jax.named_scope("gather_y2#0"):
        gather_y2(0)
    with jax.named_scope("gather_y2#1"):
        gather_y2(1)
    with jax.named_scope("halo_last#0"):
        halo_last(0)
    with jax.named_scope("forward_pair#0"):
        forward_pair(0)
    with jax.named_scope("relay_c"):
        relay_c()
    with jax.named_scope("gather_y3"):
        gather_y3()
    with jax.named_scope("project#0"):
        project(0)
    with jax.named_scope("project#1"):
        project(1)
    with jax.named_scope("relay_d"):
        relay_d()
    with jax.named_scope("weight#0"):
        weight(0)
    with jax.named_scope("project#2"):
        project(2)
    with jax.named_scope("project#3"):
        project(3)
    with jax.named_scope("backward#0"):
        backward(0, act_scale)
    with jax.named_scope("relay_e"):
        relay_e()
    with jax.named_scope("halo_last#1"):
        halo_last(1)
    with jax.named_scope("forward_pair#1"):
        forward_pair(1)
    with jax.named_scope("reduce_y#0"):
        reduce_y(0)
    with jax.named_scope("backward#1"):
        backward(1, act_scale)
    with jax.named_scope("weight#1"):
        weight(1)
    with jax.named_scope("combine#0"):
        combine(0)
    with jax.named_scope("halo_relay#3"):
        halo_relay(3)
    with jax.named_scope("halo_last#2"):
        halo_last(2)
    with jax.named_scope("forward_pair#2"):
        forward_pair(2)
    with jax.named_scope("backward#2"):
        backward(2, act_scale)
    with jax.named_scope("reduce_y2#0"):
        reduce_y2(0)
    with jax.named_scope("reduce_y#1"):
        reduce_y(1)
    with jax.named_scope("halo_last#3"):
        halo_last(3)
    with jax.named_scope("forward_pair#3"):
        forward_pair(3)
    with jax.named_scope("weight#2"):
        weight(2)
    with jax.named_scope("backward#3"):
        backward(3, act_scale)
    with jax.named_scope("combine#1"):
        combine(1)
    with jax.named_scope("weight#3"):
        weight(3)
    with jax.named_scope("reduce_y#2"):
        reduce_y(2)
    with jax.named_scope("reduce_y#3"):
        reduce_y(3)
    with jax.named_scope("reduce_y2#1"):
        reduce_y2(1)
    with jax.named_scope("combine#2"):
        combine(2)
    with jax.named_scope("reduce_y3#0"):
        reduce_y3(0)
    with jax.named_scope("reduce_y2#2"):
        reduce_y2(2)
    with jax.named_scope("reduce_y3#1"):
        reduce_y3(1)
    with jax.named_scope("reduce_y2#3"):
        reduce_y2(3)
    with jax.named_scope("reduce_y3#2"):
        reduce_y3(2)
    with jax.named_scope("combine#3"):
        combine(3)
    with jax.named_scope("reduce_y3#3"):
        reduce_y3(3)
    with jax.named_scope("reduce_z#0"):
        reduce_z(0)
    with jax.named_scope("reduce_z#1"):
        reduce_z(1)
    with jax.named_scope("reduce_z#2"):
        reduce_z(2)
    with jax.named_scope("reduce_z#3"):
        reduce_z(3)
    with jax.named_scope("finish#0"):
        finish(0, act_scale)
    with jax.named_scope("finish#1"):
        finish(1, act_scale)
    with jax.named_scope("finish#2"):
        finish(2, act_scale)
    with jax.named_scope("reduce_dp"):
        reduce_dp()
    with jax.named_scope("finish#3"):
        finish(3, act_scale)
    with jax.named_scope("reduce_swap"):
        reduce_swap(weight_scale)
    with jax.named_scope("rms"):
        rms()
    with jax.named_scope("reduce_end"):
        reduce_end()
    with jax.named_scope("drain"):
        for n, src in sent.values():
            pltpu.make_async_remote_copy(
                src_ref=src, dst_ref=src, send_sem=ssem.at[n], recv_sem=rsem.at[n],
                device_id=cp, device_id_type=MESH,
            ).wait_send()


def publish(*refs):
    given, results, sem = refs[:5], refs[5:10], refs[10]
    rows = TOK // 4
    pieces = [(n, r) for n in range(3) for r in range(4)]
    stores = [
        pltpu.make_async_copy(
            given[n].at[pl.ds(r * rows, rows)], results[n].at[pl.ds(r * rows, rows)], sem.at[4 * n + r]
        )
        for n, r in pieces
    ]
    stores.append(pltpu.make_async_copy(given[3], results[3], sem.at[12]))
    for store in stores:
        store.start()
    results[4][0, 0] = given[4][0, 0]
    for store in stores:
        store.wait()


def shards(queries, keys, values, out_grad, out_weight, seq_len):
    vm = pl.BlockSpec(memory_space=pltpu.VMEM)
    scratch = [
        ((8, HD), F32),
        ((32, 2, 16, D_OUT), BF16),
        ((TOK, 1024), BF16),
        ((TOK, 1024), BF16),
        ((TOK, 1024), BF16),
        ((TOK, 1024), BF16),
        ((TOK, D_OUT), BF16),
        ((TOK, D_OUT), BF16),
        ((HEADS, TOK, HD), BF16),
        ((KV_HEADS, TOK, HD), BF16),
        ((KV_HEADS, 2, TOK, HD), BF16),
        ((KV_HEADS, TOK, HD), BF16),
        ((HEADS, 3, TOK, TOK), BF16),
        ((HEADS, 3, TOK, TOK), BF16),
        ((8, 2, 16, D_OUT), F32),
        ((KV_HEADS, 8, 16, D_OUT), F32),
        ((KV_HEADS, 8, 16, D_OUT), BF16),
        ((KV_HEADS, 8, 16, D_OUT), BF16),
        ((6, 4, 16, D_OUT), BF16),
        ((6, 4, 16, D_OUT), BF16),
        ((8, 16, D_OUT), BF16),
        ((8, 16, D_OUT), BF16),
        ((16, D_OUT), BF16),
        ((16, D_OUT), BF16),
        ((16, D_OUT), F32),
        ((16, D_OUT), F32),
        ((KV_HEADS, 2, TOK, HD), BF16),
        ((KV_HEADS, 2, TOK, HD), BF16),
        ((KV_HEADS, 2, TOK, HD), BF16),
        ((KV_HEADS, 2, TOK, HD), BF16),
        ((KV_HEADS, 2, TOK, HD), F32),
        ((KV_HEADS, 2, TOK, HD), F32),
        ((3, 8, 128), jnp.int32),
        ((8, 8, 128), F32),
        ((32, 8, 128), F32),
    ]
    dq, dk, dv, dw, rms = pl.pallas_call(
        body,
        out_shape=(
            pltpu.VMEM((TOK, 2048), BF16),
            pltpu.VMEM((TOK, 1024), BF16),
            pltpu.VMEM((TOK, 1024), BF16),
            pltpu.VMEM((2, 16, D_OUT), F32),
            jax.ShapeDtypeStruct((1, 1), F32),
        ),
        in_specs=[pl.BlockSpec(memory_space=pltpu.SMEM)] + [vm] * 6,
        out_specs=[vm] * 4 + [pl.BlockSpec(memory_space=pltpu.SMEM)],
        scratch_shapes=[pltpu.VMEM(s, d) for s, d in scratch]
        + [pltpu.SemaphoreType.DMA((CHANNELS,)), pltpu.SemaphoreType.DMA((CHANNELS,))],
        compiler_params=pltpu.CompilerParams(
            collective_id=0, has_side_effects=True, vmem_limit_bytes=54 * 2**20
        ),
        name="band",
    )(
        seq_len,
        queries[0],
        keys[0],
        values[0],
        out_grad[0],
        out_weight.reshape(2, 16, D_OUT),
        jnp.full((8, 128), seq_len[0], jnp.int32),
    )
    shapes = [((TOK, 2048), BF16), ((TOK, 1024), BF16), ((TOK, 1024), BF16), ((2, 16, D_OUT), F32)]
    anywhere = pl.BlockSpec(memory_space=pl.ANY)
    scalar = pl.BlockSpec(memory_space=pltpu.SMEM)
    dq, dk, dv, dw, rms = pl.pallas_call(
        publish,
        out_shape=[jax.ShapeDtypeStruct(a, d) for a, d in shapes + [((1, 1), F32)]],
        in_specs=[vm] * 4 + [scalar],
        out_specs=[anywhere] * 4 + [scalar],
        scratch_shapes=[pltpu.SemaphoreType.DMA((13,))],
        name="publish",
    )(*[pltpu.with_memory_space_constraint(a, pltpu.VMEM) for a in (dq, dk, dv, dw)], rms)
    return dq[None], dk[None], dv[None], dw.reshape(32, D_OUT), rms.reshape(())


def solution(mesh):
    split = Mesh(mesh.devices.reshape(4, 2, 8, 2, 2), AXES)
    rows = P(DP, SEQ, None)
    return jax.shard_map(
        shards,
        mesh=split,
        in_specs=(rows, rows, rows, rows, P(SEQ, None), P(DP)),
        out_specs=(rows, rows, rows, P(SEQ, None), P()),
        check_vma=False,
    )
```

```python
import jax
import jax.numpy as jnp
from jax import lax
from jax.experimental import pallas as pl
from jax.experimental.pallas import tpu as pltpu
from jax.sharding import Mesh
from jax.sharding import PartitionSpec as P

HEADS = 8
KV_HEADS = 4
GROUP = HEADS // KV_HEADS
HD = 256
D_OUT = 1792
WINDOW = 512
TOK = 256
SEQ = ("sy", "sx", "sz")
DP = ("dx", "dc")
AXES = ("sy", "sx", "sz", "dx", "dc")
N_DEV_SEQ = 64
SLOTS = 4 * 16384

SCALE = 0.0625
CAP = 50.0
LOG2E = 1.4426950408889634
CHANNELS = 78
OFFSETS = [(a, b, d) for a in range(4) for b in range(4) for d in range(2) if a + b + d > 0]

F32 = jnp.float32
BF16 = jnp.bfloat16
MESH = pl.DeviceIdType.MESH


def dot_nt(a, b):
    return lax.dot_general(a, b, (((1,), (1,)), ((), ())), preferred_element_type=F32)


def dot_nn(a, b):
    return lax.dot_general(a, b, (((1,), (0,)), ((), ())), preferred_element_type=F32)


def dot_tn(a, b):
    return lax.dot_general(a, b, (((0,), (0,)), ((), ())), preferred_element_type=F32)


def col(n):
    return pl.ds(n * HD, HD)


def body(
    len_ref, q_ref, k_ref, v_ref, og_ref, w_ref,
    dq_ref, dk_ref, dv_ref, dw_ref, rms_ref,
    sq_ref, wf, k1, k2, v1, v2, mk, mk2, at, at2, ga, gs, pb, pw, tw, dwm, sdb, rdb, ysb, yrb, zsb, zrb,
    fsb, frb, hsb, hrb, c2s, c2r, cms, cmr, c1, c0, lt_ref, lts, tz, tp, ssem, rsem,
):
    y, xl, z, xh, c = (lax.axis_index(a) for a in AXES)
    oc = 1 - c
    pos = (y * 2 + xl) * 8 + z

    def at_seq(s):
        return (lax.div(s, 16), lax.rem(lax.div(s, 8), 2), lax.rem(s, 8), xh, c)

    def mod(a, n):
        return lax.rem(a, n)

    right = at_seq(mod(pos + 1, N_DEV_SEQ))
    left = at_seq(mod(pos + N_DEV_SEQ - 1, N_DEV_SEQ))
    yn = (mod(y + 1, 4), xl, z, xh, c)
    yp = (mod(y + 3, 4), xl, z, xh, c)
    xr = (y, 1 - xl, z, mod(xh + xl, 2), c)
    xp = (y, 1 - xl, z, mod(xh + 1 - xl, 2), c)
    x2 = (y, xl, z, 1 - xh, c)
    x2o = (y, xl, z, 1 - xh, oc)
    cp = (y, xl, z, xh, oc)
    pair = (y, 1 - xl, z, 1 - xh, c)

    def zpeer(k):
        return (y, xl, mod(z + k, 8), xh, c)

    ids = {}
    sent = {}

    def channel(name):
        return ids.setdefault(name, len(ids))

    def send(name, src, dst, dev):
        n = channel(name)
        d = pltpu.make_async_remote_copy(
            src_ref=src, dst_ref=dst, send_sem=ssem.at[n], recv_sem=rsem.at[n],
            device_id=dev, device_id_type=MESH,
        )
        d.start()
        sent[name] = (n, src)

    def recv(name, dst):
        n = channel(name)
        pltpu.make_async_remote_copy(
            src_ref=dst, dst_ref=dst, send_sem=ssem.at[n], recv_sem=rsem.at[n],
            device_id=cp, device_id_type=MESH,
        ).wait_recv()

    barrier = pltpu.get_barrier_semaphore()
    x = xh * 2 + xl

    def plane(dy, dx, dc):
        there = mod(x + dx, 4)
        return (mod(y + dy, 4), mod(there, 2), z, lax.div(there, 2), mod(c + dc, 2))

    def plane_slot(dy, dx, dc):
        return (mod(y + dy + 4, 4) * 4 + mod(x + dx + 4, 4)) * 2 + mod(c + dc, 2)

    peers = [zpeer(k) for k in range(1, 8)] + [plane(*o) for o in OFFSETS] + [right, left]
    for dev in peers:
        pl.semaphore_signal(barrier, inc=1, device_id=dev, device_id_type=MESH)
    pl.semaphore_wait(barrier, len(peers))

    def unit(j):
        return mod(y + j, 4)

    def part(u, p, h):
        return wf.at[pl.ds(8 * u + 4 * p, 4), h]

    ours = [[[part(unit(j), p, h) for h in (c, oc)] for p in range(2)] for j in range(4)]

    one_way = jnp.logical_and(z == 0, xl == 0)

    def spread(j, p):
        ref = ours[j][p][0]
        send(f"d{j}{p}", ref, ref, cp)

    def gather_z():
        for k in (1, 7, 6, 2, 3, 5, 4):
            send(f"z{k}", w_ref.at[c], wf.at[8 * y + (9 - k) % 8, c], zpeer(k))
        wf[8 * y + 1, c] = w_ref[c]

    def gather_y(p):
        for k in ((1, 7, 6), (2, 3, 5, 4))[p]:
            recv(f"z{k}", wf.at[8 * y + (9 - k) % 8, c])
        ref = ours[0][p][0]
        if p == 0:
            send("ya0", ref, ref, yn)
        else:

            @pl.when(jnp.logical_not(one_way))
            def _():
                send("ya1", ref, ref, yn)

        send(f"yb{p}", ref, ref, yp)
        spread(0, p)

    def gather_y0():
        ref = ours[3][0][0]
        recv("ya0", ref)

        @pl.when(jnp.logical_not(one_way))
        def _():
            send("yf0", ref, ref, yn)

        spread(3, 0)
        ref = ours[1][0][0]
        recv("yb0", ref)

        @pl.when(one_way)
        def _():
            send("yf0", ref, ref, yp)

        spread(1, 0)

    def gather_ya1():
        recv("ya1", ours[3][1][0])
        spread(3, 1)

    def gather_y1():
        ref = ours[1][1][0]
        recv("yb1", ref)
        send("yf1", ref, ref, yp)
        spread(1, 1)
        pl.when(jnp.logical_not(one_way))(gather_ya1)

    def gather_y2(p):
        ref = ours[2][p][0]
        recv(f"yf{p}", ref)
        if p == 1:

            @pl.when(one_way)
            def _():
                send("ya1", ref, ref, yp)

        spread(2, p)

    def gather_y3():
        pl.when(one_way)(gather_ya1)

    def halo_own(kh):
        send(f"ok{kh}", k_ref.at[:, col(kh)], k1.at[:, col(kh)], right)
        send(f"ov{kh}", v_ref.at[:, col(kh)], v1.at[:, col(kh)], right)

    def halo_relay(kh):
        recv(f"ok{kh}", k1.at[:, col(kh)])
        send(f"fk{kh}", k1.at[:, col(kh)], k2.at[:, col(kh)], right)
        recv(f"ov{kh}", v1.at[:, col(kh)])
        send(f"fv{kh}", v1.at[:, col(kh)], v2.at[:, col(kh)], right)

    holds = xl * lax.div(z, 7)

    def relay_a():
        pl.when(z == 0)(lambda: [halo_own(1), halo_relay(0), halo_own(2)] and None)
        pl.when((holds == 0) & (z > 0))(lambda: [halo_relay(0), halo_own(1)] and None)

    def relay_b():
        pl.when(holds == 1)(lambda: [halo_relay(0), halo_own(1)] and None)

    def relay_c():
        pl.when(z == 0)(lambda: halo_own(3))
        pl.when(z > 0)(lambda: [halo_relay(1), halo_own(2)] and None)

    def relay_d():
        pl.when(z == 0)(lambda: halo_relay(1))

    def relay_e():
        halo_relay(2)
        pl.when(z > 0)(lambda: halo_own(3))

    def halo_last(kh):
        recv(f"fk{kh}", k2.at[:, col(kh)])
        recv(f"fv{kh}", v2.at[:, col(kh)])

    def lengths_send():
        send("l0", lt_ref, lts.at[0], cp)
        send("l1", lt_ref, lts.at[1], x2)
        send("l2", lt_ref, lts.at[2], x2o)

    def lengths():
        for n in range(3):
            recv(f"l{n}", lts.at[n])
        total = (lt_ref[...] + lts[0] + lts[1] + lts[2]).astype(F32)[0:1, 0:1]
        return SLOTS / total, lax.rsqrt(total)

    def masked():
        row = lax.broadcasted_iota(jnp.int32, (TOK, 1), 0)
        mk[...] = jnp.where(row < len_ref[0] - pos * TOK, og_ref[...], jnp.zeros((), BF16))
        send("xm", mk, mk2, pair)

    def forward(h):
        kh = h // GROUP
        q = q_ref[:, col(h)]
        row = lax.broadcasted_iota(jnp.int32, (TOK, TOK), 0)
        cl = lax.broadcasted_iota(jnp.int32, (TOK, TOK), 1)
        far = jnp.where(pos >= 2, 0, 2 * TOK)
        near = jnp.where(pos >= 1, 0, 2 * TOK)
        allowed = (cl - row > far, cl >= near, cl <= row)
        es, ws = [], []
        total = jnp.zeros((TOK, 1), F32)
        for b, ref in enumerate((k2, k1, k_ref)):
            t = jnp.tanh(dot_nt(q, ref[:, col(kh)]) * (SCALE / CAP))
            e = jnp.where(allowed[b], jnp.exp2(t * (CAP * LOG2E)), 0.0)
            total = total + jnp.sum(e, axis=1, keepdims=True)
            es.append(e)
            ws.append(e * (SCALE - SCALE * (t * t)))
        inv = 1.0 / total
        out = jnp.zeros((TOK, HD), F32)
        for b, ref in enumerate((v2, v1, v_ref)):
            p = (es[b] * inv).astype(BF16)
            pb[h, b] = p
            pw[h, b] = (ws[b] * inv).astype(BF16)
            out = out + dot_nn(p, ref[:, col(kh)])
        at[h] = out.astype(BF16)

    def forward_pair(kh):
        for g in range(GROUP):
            forward(kh * GROUP + g)
        send(f"xa{kh}", at.at[kh * GROUP + 1 - xl], at2.at[kh], pair)

    def project(kh):
        if kh == 0:
            recv("xm", mk2)
        for j in range(4):

            @pl.when(mod(kh - y + 4, 4) == j)
            def _():
                for p in range(2):
                    recv(f"d{j}{p}", ours[j][p][1])

        blocks = [wf[8 * kh + mod(n + 9 - z, 8)].reshape(32, D_OUT) for n in range(8)]
        wh = jnp.concatenate(blocks, axis=0)
        gs[kh] = dot_nt(mk2[...], wh).astype(BF16)
        send(f"xg{kh}", gs.at[kh], ga.at[kh, xl], pair)
        ga[kh, xl] = dot_nt(mk[...], wh).astype(BF16)

    def weight(kh):
        recv(f"xa{kh}", at2.at[kh])
        total = dot_tn(at[kh * GROUP + xl], mk[...]) + dot_tn(at2[kh], mk2[...])
        tw[...] = total.reshape(8, 2, 16, D_OUT)
        sdb[kh] = tw[:, oc].astype(BF16)
        dwm[kh] = tw[:, c]
        send(f"rd{kh}", sdb.at[kh], rdb.at[kh], cp)

    def mine(kh, p):
        return dwm[kh, pl.ds(4 * p, 4)]

    y_refs = [ysb.at[n] for n in range(6)]

    def y_send(n, value, dev):
        ysb[n] = value.astype(BF16)
        send(f"r{n}", y_refs[n], yrb.at[n], dev)

    def role(kh, j):
        return pl.when(mod(kh - y + 4, 4) == j)

    one = xl * lax.div(z, 7)

    def role_if(kh, j, flag):
        return pl.when(jnp.logical_and(mod(kh - y + 4, 4) == j, one == flag))

    def y_relay(n, kh, p):
        recv(f"r{n}", yrb.at[n])
        return mine(kh, p) + yrb[n].astype(F32)

    def reduce_y(kh):
        recv(f"rd{kh}", rdb.at[kh])
        dwm[kh] = dwm[kh] + rdb[kh].astype(F32)

        @role_if(kh, 2, 0)
        def _():
            y_send(0, mine(kh, 0), yn)
            y_send(1, mine(kh, 1), yp)

        @role_if(kh, 1, 0)
        def _():
            y_send(2, mine(kh, 1), yn)

        @role_if(kh, 3, 0)
        def _():
            y_send(3, mine(kh, 0), yp)

        @role_if(kh, 3, 1)
        def _():
            y_send(0, mine(kh, 0), yn)
            y_send(1, mine(kh, 1), yn)

    def reduce_y2(kh):
        @role_if(kh, 1, 0)
        def _():
            y_send(4, y_relay(0, kh, 0), yn)

        @role_if(kh, 3, 0)
        def _():
            y_send(5, y_relay(1, kh, 1), yp)

        @role_if(kh, 2, 1)
        def _():
            y_send(2, y_relay(0, kh, 0), yn)
            y_send(3, y_relay(1, kh, 1), yn)

    def reduce_y3(kh):
        @role_if(kh, 1, 1)
        def _():
            y_send(4, y_relay(2, kh, 0), yn)
            y_send(5, y_relay(3, kh, 1), yn)

    z_refs = [zsb.at[mod(z + k, 8)] for k in range(8)]

    def reduce_z(kh):
        @role_if(kh, 0, 0)
        def _():
            recv("r3", yrb.at[3])
            recv("r2", yrb.at[2])
            for p in range(2):
                rows = pl.ds(4 * p, 4)
                dwm[kh, rows] = mine(kh, p) + yrb[3 - p].astype(F32)

        for p in range(2):
            rows = pl.ds(4 * p, 4)

            @role(kh, 0)
            def _():
                total = y_relay(4 + p, kh, p)
                dwm[kh, rows] = total
                zsb[rows] = total.astype(BF16)

            for k in range(1, 8):

                @pl.when(jnp.logical_and(kh == y, lax.div(mod(z + k, 8), 4) == p))
                def _():
                    send(f"rz{k}", z_refs[k], zrb.at[k], zpeer(k))

    def reduce_dp():
        total = dwm[y, z]
        for k in range(1, 8):
            recv(f"rz{k}", zrb.at[k])
            total = total + zrb[k].astype(F32)
        fsb[...] = total.astype(BF16)
        send("f", fsb, frb, x2)

    def reduce_swap(weight_scale):
        recv("f", frb)
        total = (fsb[...].astype(F32) + frb[...].astype(F32)) * weight_scale
        hsb[...] = total
        send("h", hsb, hrb, cp)
        dw_ref[c] = total
        square = total * total * 0.5
        acc = sq_ref[...]
        for n in range(D_OUT // HD):
            acc = acc + square[0:8, n * HD : (n + 1) * HD] + square[8:16, n * HD : (n + 1) * HD]
        sq_ref[...] = acc

    def reduce_end():
        recv("h", hrb)
        dw_ref[oc] = hrb[...]

    def squares(x):
        sq_ref[...] += jnp.sum((x * x).reshape(TOK // 8, 8, HD), axis=0)

    def backward(kh, act_scale):
        recv(f"xg{kh}", ga.at[kh, 1 - xl])
        sk = [None] * 3
        sv = [None] * 3
        for g in range(GROUP):
            h = kh * GROUP + g
            q = q_ref[:, col(h)]
            gh = ga[kh, g]
            delta = jnp.sum(gh.astype(F32) * at[h].astype(F32), axis=1, keepdims=True)
            dq = jnp.zeros((TOK, HD), F32)
            for b, (kr, vr) in enumerate(((k2, v2), (k1, v1), (k_ref, v_ref))):
                dp = dot_nt(gh, vr[:, col(kh)])
                ds = (pw[h, b].astype(F32) * (dp - delta)).astype(BF16)
                dq = dq + dot_nn(ds, kr[:, col(kh)])
                dk = dot_tn(ds, q)
                dv = dot_tn(pb[h, b], gh)
                sk[b] = dk if g == 0 else sk[b] + dk
                sv[b] = dv if g == 0 else sv[b] + dv
            dq = dq * act_scale
            squares(dq)
            dq_ref[:, col(h)] = dq.astype(BF16)
        c2s[kh, 0] = sk[0].astype(BF16)
        c2s[kh, 1] = sv[0].astype(BF16)
        send(f"b{kh}", c2s.at[kh], c2r.at[kh], left)
        c1[kh, 0] = sk[1]
        c1[kh, 1] = sv[1]
        c0[kh, 0] = sk[2]
        c0[kh, 1] = sv[2]

    def combine(kh):
        recv(f"b{kh}", c2r.at[kh])
        cms[kh] = (c1[kh] + c2r[kh].astype(F32)).astype(BF16)
        send(f"m{kh}", cms.at[kh], cmr.at[kh], left)

    def finish(kh, act_scale):
        recv(f"m{kh}", cmr.at[kh])
        for n, ref in enumerate((dk_ref, dv_ref)):
            total = (c0[kh, n] + cmr[kh, n].astype(F32)) * act_scale
            squares(total)
            ref[:, col(kh)] = total.astype(BF16)

    def everyone(name, buf, at_me, value, devs):
        buf[at_me] = value
        n = channel(name)
        for dev in devs:
            pltpu.make_async_remote_copy(
                src_ref=buf.at[at_me], dst_ref=buf.at[at_me], send_sem=ssem.at[n],
                recv_sem=rsem.at[n], device_id=dev, device_id_type=MESH,
            ).start()
        sent[name] = (n, buf.at[pl.ds(0, len(devs))])

    def heard(name, buf):
        recv(name, buf.at[pl.ds(0, buf.shape[0] - 1)])
        total = buf[0]
        for n in range(1, buf.shape[0]):
            total = total + buf[n]
        return total

    def rms():
        own = jnp.sum(jnp.sum(sq_ref[...], axis=0, keepdims=True), axis=1, keepdims=True)
        own = jnp.broadcast_to(own, (8, 128))
        everyone("sz", tz, z, own, [zpeer(k) for k in range(1, 8)])
        total = heard("sz", tz)
        everyone("sp", tp, plane_slot(0, 0, 0), total, [plane(*o) for o in OFFSETS])
        total = heard("sp", tp)
        entries = SLOTS * (HEADS + 2 * KV_HEADS) * HD + HEADS * HD * D_OUT
        rms_ref[0, 0] = jnp.sqrt(total * (1.0 / entries))[0, 0]

    lt_ref[...] = jnp.full((8, 128), len_ref[0], jnp.int32)
    sq_ref[...] = jnp.zeros_like(sq_ref)
    with jax.named_scope("gather_z"):
        gather_z()
    with jax.named_scope("halo_own#0"):
        halo_own(0)
    with jax.named_scope("masked"):
        masked()
    with jax.named_scope("lengths_send"):
        lengths_send()
    with jax.named_scope("gather_y#0"):
        gather_y(0)
    with jax.named_scope("lengths"):
        act_scale, weight_scale = lengths()
    with jax.named_scope("gather_y#1"):
        gather_y(1)
    with jax.named_scope("gather_y0"):
        gather_y0()
    with jax.named_scope("relay_a"):
        relay_a()
    with jax.named_scope("gather_y1"):
        gather_y1()
    with jax.named_scope("relay_b"):
        relay_b()
    with jax.named_scope("gather_y2#0"):
        gather_y2(0)
    with jax.named_scope("gather_y2#1"):
        gather_y2(1)
    with jax.named_scope("halo_last#0"):
        halo_last(0)
    with jax.named_scope("forward_pair#0"):
        forward_pair(0)
    with jax.named_scope("relay_c"):
        relay_c()
    with jax.named_scope("gather_y3"):
        gather_y3()
    with jax.named_scope("project#0"):
        project(0)
    with jax.named_scope("project#1"):
        project(1)
    with jax.named_scope("relay_d"):
        relay_d()
    with jax.named_scope("weight#0"):
        weight(0)
    with jax.named_scope("project#2"):
        project(2)
    with jax.named_scope("project#3"):
        project(3)
    with jax.named_scope("backward#0"):
        backward(0, act_scale)
    with jax.named_scope("relay_e"):
        relay_e()
    with jax.named_scope("halo_last#1"):
        halo_last(1)
    with jax.named_scope("forward_pair#1"):
        forward_pair(1)
    with jax.named_scope("reduce_y#0"):
        reduce_y(0)
    with jax.named_scope("backward#1"):
        backward(1, act_scale)
    with jax.named_scope("weight#1"):
        weight(1)
    with jax.named_scope("combine#0"):
        combine(0)
    with jax.named_scope("halo_relay#3"):
        halo_relay(3)
    with jax.named_scope("halo_last#2"):
        halo_last(2)
    with jax.named_scope("forward_pair#2"):
        forward_pair(2)
    with jax.named_scope("backward#2"):
        backward(2, act_scale)
    with jax.named_scope("reduce_y2#0"):
        reduce_y2(0)
    with jax.named_scope("reduce_y#1"):
        reduce_y(1)
    with jax.named_scope("halo_last#3"):
        halo_last(3)
    with jax.named_scope("forward_pair#3"):
        forward_pair(3)
    with jax.named_scope("weight#2"):
        weight(2)
    with jax.named_scope("backward#3"):
        backward(3, act_scale)
    with jax.named_scope("combine#1"):
        combine(1)
    with jax.named_scope("weight#3"):
        weight(3)
    with jax.named_scope("reduce_y#2"):
        reduce_y(2)
    with jax.named_scope("reduce_y#3"):
        reduce_y(3)
    with jax.named_scope("reduce_y2#1"):
        reduce_y2(1)
    with jax.named_scope("reduce_y3#0"):
        reduce_y3(0)
    with jax.named_scope("reduce_y2#2"):
        reduce_y2(2)
    with jax.named_scope("combine#2"):
        combine(2)
    with jax.named_scope("reduce_y2#3"):
        reduce_y2(3)
    with jax.named_scope("reduce_y3#1"):
        reduce_y3(1)
    with jax.named_scope("reduce_y3#2"):
        reduce_y3(2)
    with jax.named_scope("combine#3"):
        combine(3)
    with jax.named_scope("reduce_y3#3"):
        reduce_y3(3)
    with jax.named_scope("reduce_z#3"):
        reduce_z(3)
    with jax.named_scope("reduce_z#0"):
        reduce_z(0)
    with jax.named_scope("reduce_z#1"):
        reduce_z(1)
    with jax.named_scope("reduce_z#2"):
        reduce_z(2)
    with jax.named_scope("finish#0"):
        finish(0, act_scale)
    with jax.named_scope("finish#1"):
        finish(1, act_scale)
    with jax.named_scope("finish#2"):
        finish(2, act_scale)
    with jax.named_scope("reduce_dp"):
        reduce_dp()
    with jax.named_scope("finish#3"):
        finish(3, act_scale)
    with jax.named_scope("reduce_swap"):
        reduce_swap(weight_scale)
    with jax.named_scope("rms"):
        rms()
    with jax.named_scope("reduce_end"):
        reduce_end()
    assert len(ids) <= CHANNELS
    with jax.named_scope("drain"):
        for n, src in sent.values():
            pltpu.make_async_remote_copy(
                src_ref=src, dst_ref=src, send_sem=ssem.at[n], recv_sem=rsem.at[n],
                device_id=cp, device_id_type=MESH,
            ).wait_send()


def publish(*refs):
    given, results, sem = refs[:5], refs[5:10], refs[10]
    rows = TOK // 4
    pieces = [(n, r) for n in range(3) for r in range(4)]
    stores = [
        pltpu.make_async_copy(
            given[n].at[pl.ds(r * rows, rows)], results[n].at[pl.ds(r * rows, rows)], sem.at[4 * n + r]
        )
        for n, r in pieces
    ]
    stores.append(pltpu.make_async_copy(given[3], results[3], sem.at[12]))
    for store in stores:
        store.start()
    results[4][0, 0] = given[4][0, 0]
    for store in stores:
        store.wait()


def shards(queries, keys, values, out_grad, out_weight, seq_len):
    vm = pl.BlockSpec(memory_space=pltpu.VMEM)
    scratch = [
        ((8, HD), F32),
        ((32, 2, 16, D_OUT), BF16),
        ((TOK, 1024), BF16),
        ((TOK, 1024), BF16),
        ((TOK, 1024), BF16),
        ((TOK, 1024), BF16),
        ((TOK, D_OUT), BF16),
        ((TOK, D_OUT), BF16),
        ((HEADS, TOK, HD), BF16),
        ((KV_HEADS, TOK, HD), BF16),
        ((KV_HEADS, 2, TOK, HD), BF16),
        ((KV_HEADS, TOK, HD), BF16),
        ((HEADS, 3, TOK, TOK), BF16),
        ((HEADS, 3, TOK, TOK), BF16),
        ((8, 2, 16, D_OUT), F32),
        ((KV_HEADS, 8, 16, D_OUT), F32),
        ((KV_HEADS, 8, 16, D_OUT), BF16),
        ((KV_HEADS, 8, 16, D_OUT), BF16),
        ((6, 4, 16, D_OUT), BF16),
        ((6, 4, 16, D_OUT), BF16),
        ((8, 16, D_OUT), BF16),
        ((8, 16, D_OUT), BF16),
        ((16, D_OUT), BF16),
        ((16, D_OUT), BF16),
        ((16, D_OUT), F32),
        ((16, D_OUT), F32),
        ((KV_HEADS, 2, TOK, HD), BF16),
        ((KV_HEADS, 2, TOK, HD), BF16),
        ((KV_HEADS, 2, TOK, HD), BF16),
        ((KV_HEADS, 2, TOK, HD), BF16),
        ((KV_HEADS, 2, TOK, HD), F32),
        ((KV_HEADS, 2, TOK, HD), F32),
        ((8, 128), jnp.int32),
        ((3, 8, 128), jnp.int32),
        ((8, 8, 128), F32),
        ((32, 8, 128), F32),
    ]
    dq, dk, dv, dw, rms = pl.pallas_call(
        body,
        out_shape=(
            pltpu.VMEM((TOK, 2048), BF16),
            pltpu.VMEM((TOK, 1024), BF16),
            pltpu.VMEM((TOK, 1024), BF16),
            pltpu.VMEM((2, 16, D_OUT), F32),
            jax.ShapeDtypeStruct((1, 1), F32),
        ),
        in_specs=[pl.BlockSpec(memory_space=pltpu.SMEM)] + [vm] * 5,
        out_specs=[vm] * 4 + [pl.BlockSpec(memory_space=pltpu.SMEM)],
        scratch_shapes=[pltpu.VMEM(s, d) for s, d in scratch]
        + [pltpu.SemaphoreType.DMA((CHANNELS,)), pltpu.SemaphoreType.DMA((CHANNELS,))],
        compiler_params=pltpu.CompilerParams(
            collective_id=0, has_side_effects=True, vmem_limit_bytes=54 * 2**20
        ),
        name="band",
    )(
        seq_len,
        queries[0],
        keys[0],
        values[0],
        out_grad[0],
        out_weight.reshape(2, 16, D_OUT),
    )
    shapes = [((TOK, 2048), BF16), ((TOK, 1024), BF16), ((TOK, 1024), BF16), ((2, 16, D_OUT), F32)]
    anywhere = pl.BlockSpec(memory_space=pl.ANY)
    scalar = pl.BlockSpec(memory_space=pltpu.SMEM)
    dq, dk, dv, dw, rms = pl.pallas_call(
        publish,
        out_shape=[jax.ShapeDtypeStruct(a, d) for a, d in shapes + [((1, 1), F32)]],
        in_specs=[vm] * 4 + [scalar],
        out_specs=[anywhere] * 4 + [scalar],
        scratch_shapes=[pltpu.SemaphoreType.DMA((13,))],
        name="publish",
    )(*[pltpu.with_memory_space_constraint(a, pltpu.VMEM) for a in (dq, dk, dv, dw)], rms)
    return dq[None], dk[None], dv[None], dw.reshape(32, D_OUT), rms.reshape(())


def solution(mesh):
    split = Mesh(mesh.devices.reshape(4, 2, 8, 2, 2), AXES)
    rows = P(DP, SEQ, None)
    return jax.shard_map(
        shards,
        mesh=split,
        in_specs=(rows, rows, rows, rows, P(SEQ, None), P(DP)),
        out_specs=(rows, rows, rows, P(SEQ, None), P()),
        check_vma=False,
    )
```
